256 devices in a mesh: row: 8 (over y, core), col: 32 (over z, x).
Axes of the slice: x: 4, y: 4, z: 8, core: 2. Of those that a mesh axis runs over, the one named last changes fastest.
Arguments:
- fock: float32 [2, 8192, 8192], P(None, 'row', 'col'), may hold values from -1.1875 to 1.1875, as said below
- density: float32 [2, 8192, 8192], P(None, 'row', 'col'), may hold values from -1.09375 to 1.09375, as said below
- probe: float32 [2, 8192, 128], P(None, 'col'), may hold values from -6 to 6
Outputs:
- propagated: float32 [2, 8192, 128], P(None, 'col')
The draws below stay inside these ranges and needn't reach their ends.
Inputs may be any that keep to these rules, and one draw needn't show every extreme that they name: Hermitian: fock[0] is symmetric and fock[1] antisymmetric, exactly. Hermitian: density[0] is symmetric and density[1] antisymmetric, exactly.
All inputs are finite; a program needn't handle non-finite values.
Results may differ from the reference program's by a relative error of at most 0.00011.
Values sent between devices are 32-bit elements; how exact they have to be, the bound alone decides.
A program may use at most 64 MiB of HBM per device.

```python
import jax
import jax.numpy as jnp
from jax import lax

N = 8192
M = 128
ORDER = 1


def hermitian(key, spread):
    key_real, key_imag = jax.random.split(key, 2)
    real_base = jnp.clip(jax.random.normal(key_real, (N, N), jnp.float32), -6.0, 6.0)
    imag_base = jnp.clip(jax.random.normal(key_imag, (N, N), jnp.float32), -6.0, 6.0)
    factor = spread / jnp.sqrt(2.0 * N)
    real_part = (real_base + real_base.T) * factor
    imag_part = (imag_base - imag_base.T) * factor
    return jnp.stack([real_part, imag_part])


def draw_fock(key, part):
    return hermitian(jax.random.fold_in(key, 11), 2.0)


def draw_density(key, part):
    return hermitian(jax.random.fold_in(key, 23), 1.0)


def block_scale(rng, dims, cuts, smallest, high):
    factor_of, own = 1.0, jax.random.fold_in(rng, 6)
    for position, parts in cuts:
        draws = jnp.exp(jax.random.uniform(jax.random.fold_in(own, position), (parts,), jnp.float32, smallest / len(cuts), high / len(cuts)))
        factor_of = factor_of * jnp.repeat(draws, dims[position] // parts).reshape([-1 if axis == position else 1 for axis in range(len(dims))])
    return factor_of


def gaussian(key, dims, scale, reach, cuts=(), kind=jnp.bfloat16):
    entries = jax.random.normal(key, dims, jnp.float32) * scale
    if len(cuts) > 0:
        entries = block_scale(key, dims, cuts, -0.22, 0.18) * entries
    return jnp.clip(entries, min=-reach, max=reach).astype(kind)


def setup_inputs(seed: int = 0) -> dict:
    streams_of = jax.random.split(jax.random.key(seed), 4)
    fock = draw_fock(jax.random.fold_in(streams_of[3], 71), 0)
    density = draw_density(jax.random.fold_in(streams_of[3], 71), 0)
    probe = gaussian(streams_of[2], (2, N, M), 1.0, 6.0, ((1, 32),), jnp.float32)
    return {"fock": fock, "density": density, "probe": probe}


time_step = 0.5


def complex_product(matrix, vector):
    hp = lax.Precision.HIGHEST
    real_part = jnp.dot(matrix[0], vector[0], precision=hp, preferred_element_type=jnp.float32) - jnp.dot(matrix[1], vector[1], precision=hp, preferred_element_type=jnp.float32)
    imag_part = jnp.dot(matrix[0], vector[1], precision=hp, preferred_element_type=jnp.float32) + jnp.dot(matrix[1], vector[0], precision=hp, preferred_element_type=jnp.float32)
    return jnp.stack([real_part, imag_part])


def times_imag(vector, factor):
    return jnp.stack([-factor * vector[1], factor * vector[0]])


def series(fock, start, sign):
    current = start
    total = start
    for degree in range(1, ORDER + 1):
        current = times_imag(complex_product(fock, current), sign * time_step / degree)
        total = total + current
    return total


def reference(fock, density, probe):
    first = series(fock, probe, 1.0)
    second = complex_product(density, first)
    return series(fock, second, -1.0)
```

```python
import functools

import jax
import jax.numpy as jnp
from jax import lax
from jax.experimental import pallas as pl
from jax.experimental.pallas import tpu as pltpu
from jax.sharding import PartitionSpec as P

MESH = pl.DeviceIdType.MESH
DT = 0.5
GROUPS = 2
ROWS = 1024
COLS = 256
PIECES = 8
DEPTH = 16
WIDE = PIECES * DEPTH


def split(value):
    high = value.astype(jnp.bfloat16)
    return high, (value - high.astype(jnp.float32)).astype(jnp.bfloat16)


def prepare(matrix, high, low):
    def part(i, carry):
        rows = pl.ds(pl.multiple_of(i * COLS, COLS), COLS)
        for j in range(2):
            h, l = split(matrix[j, rows, :])
            high[rows, j * COLS : (j + 1) * COLS] = h
            low[rows, j * COLS : (j + 1) * COLS] = l
        return carry

    lax.fori_loop(0, ROWS // COLS, part, 0)


def factors(phase, vector):
    real, imag = vector[:, :8], vector[:, 8:]
    if phase == 1:
        first, second = (real, imag), (-imag, real)
    else:
        dt = DT if phase == 0 else -DT
        first, second = (-dt * imag, dt * real), (-dt * real, -dt * imag)
    first = jnp.concatenate(first, axis=1).reshape(WIDE, COLS)
    second = jnp.concatenate(second, axis=1).reshape(WIDE, COLS)
    return jnp.concatenate([first, second], axis=1)


def times(high, low, matrix_high, matrix_low):
    dot = functools.partial(
        lax.dot_general,
        dimension_numbers=(((1,), (1,)), ((), ())),
        preferred_element_type=jnp.float32,
    )
    return dot(high, matrix_high) + (dot(low, matrix_high) + dot(high, matrix_low))


def kernel(
    fock_hbm, density_hbm, probe_hbm, out,
    fock, density, probe, fock_high, fock_low, density_high, density_low,
    start, chunks, relay_a, relay_b, from_left, from_right, summed, arrived, gathered,
    load_sem, x_send, x_recv, z_send, z_recv, g_send, g_recv,
):
    row, col = lax.axis_index("row"), lax.axis_index("col")
    z, x = col // 4, lax.rem(col, 4)
    right = z * 4 + lax.rem(x + 1, 4)
    left = z * 4 + lax.rem(x + 3, 4)
    home = row * 4 + x
    at_home = row == z

    loads = [
        pltpu.make_async_copy(source, target, load_sem.at[i])
        for i, (source, target) in enumerate(
            ((probe_hbm, probe), (fock_hbm, fock), (density_hbm, density))
        )
    ]
    for load in loads:
        load.start()

    barrier = pltpu.get_barrier_semaphore()

    def hello(r, c):
        pl.semaphore_signal(barrier, inc=1, device_id=(r, c), device_id_type=MESH)

    hello(row, right)
    hello(row, left)
    for j in range(1, PIECES):
        hello(lax.rem(row + j, PIECES), col)
        hello(z, lax.rem(z + j, 8) * 4 + x)

    @pl.when(jnp.logical_not(at_home))
    def _():
        hello(z, col)

    loads[0].wait()
    for j in range(2):
        turned = probe[j].T
        for g in range(GROUPS):
            start[g, :, j * 8 : (j + 1) * 8, :] = turned[g * 64 : (g + 1) * 64].reshape(PIECES, 8, COLS)
    loads[1].wait()
    prepare(fock, fock_high, fock_low)

    sends = []

    def send(source, target, send_sem, recv_sem, device):
        copy = pltpu.make_async_remote_copy(
            src_ref=source, dst_ref=target, send_sem=send_sem, recv_sem=recv_sem,
            device_id=device, device_id_type=MESH,
        )
        copy.start()
        sends.append(copy.wait_send)

    def landed(target, sem):
        pltpu.make_async_copy(target, target, sem).wait()

    A, B = pl.ds(0, 4), pl.ds(4, 4)

    def multiply(phase, g):
        if phase == 0:
            vector = start[g]
        else:
            landed(gathered.at[phase - 1, g, pl.ds(0, 7)], g_recv.at[phase - 1, g])
            vector = gathered[phase - 1, g]
        high, low = split(factors(phase, vector))
        mh, ml = (density_high, density_low) if phase == 1 else (fock_high, fock_low)
        box = chunks.at[phase, g]

        def one(slot, ahead):
            rows = pl.ds(pl.multiple_of(lax.rem(x + ahead, 4) * COLS, COLS), COLS)
            box[slot] = times(high, low, mh[rows, :], ml[rows, :]).reshape(PIECES, DEPTH, COLS)

        return box, one

    def x_ends(phase, g):
        s, r = x_send.at[phase, g], x_recv.at[phase, g]
        return s, r

    def stage_x(phase, g):
        box, one = multiply(phase, g)
        s, r = x_ends(phase, g)
        one(0, 2)
        if phase == 0 and g == 0:
            pl.semaphore_wait(barrier, 17 - at_home.astype(jnp.int32))

        send(box.at[0, A], relay_a.at[phase, g], s.at[0], r.at[0], (row, right))
        send(box.at[0, B], relay_b.at[phase, g], s.at[1], r.at[1], (row, left))
        one(1, 1)
        send(box.at[1, B], from_left.at[phase, g, B], s.at[2], r.at[2], (row, right))
        one(2, 3)
        send(box.at[2, A], from_right.at[phase, g, A], s.at[3], r.at[3], (row, left))
        one(3, 0)

    def stage_relay(phase, g):
        box = chunks.at[phase, g]
        s, r = x_ends(phase, g)
        landed(relay_a.at[phase, g], r.at[0])
        box[1, 0:4] = box[1, 0:4] + relay_a[phase, g]
        send(box.at[1, A], from_left.at[phase, g, A], s.at[4], r.at[4], (row, right))
        landed(relay_b.at[phase, g], r.at[1])
        box[2, 4:8] = box[2, 4:8] + relay_b[phase, g]
        send(box.at[2, B], from_right.at[phase, g, B], s.at[5], r.at[5], (row, left))

    def stage_z(phase, g):
        s, r = x_ends(phase, g)
        landed(from_left.at[phase, g, B], r.at[2])
        landed(from_right.at[phase, g, A], r.at[3])
        landed(from_left.at[phase, g, A], r.at[4])
        landed(from_right.at[phase, g, B], r.at[5])
        summed[phase, g] = chunks[phase, g, 3] + from_left[phase, g] + from_right[phase, g]
        s, r = z_send.at[phase, g], z_recv.at[phase, g]
        for j in range(PIECES - 1, 0, -1):
            p = lax.rem(row + j, PIECES)
            send(summed.at[phase, g, p], arrived.at[phase, g, z], s.at[j], r, (p, home))
        copy = pltpu.make_async_remote_copy(
            src_ref=summed.at[phase, g, row], dst_ref=arrived.at[phase, g, z], send_sem=s.at[0], recv_sem=r,
            device_id=(row, home), device_id_type=MESH,
        )

        @pl.when(jnp.logical_not(at_home))
        def _():
            copy.start()

        @pl.when(at_home)
        def _():
            arrived[phase, g, z] = summed[phase, g, row]

        def wait_send():
            @pl.when(jnp.logical_not(at_home))
            def _():
                copy.wait_send()

        sends.append(wait_send)

    def stage_gather(phase, g):
        @pl.when(at_home)
        def _():
            landed(arrived.at[phase, g, pl.ds(0, 7)], z_recv.at[phase, g])

        @pl.when(jnp.logical_not(at_home))
        def _():
            landed(arrived.at[phase, g], z_recv.at[phase, g])

        a = arrived.at[phase, g]
        total = ((a[0] + a[1]) + (a[2] + a[3])) + ((a[4] + a[5]) + (a[6] + a[7]))
        if phase == 0:
            total = total + start[g, row]
        if phase == 2:
            total = total + gathered[1, g, row]
        mine = gathered.at[phase, g, row]
        mine[...] = total
        for j in range(1, PIECES):
            send(mine, mine, g_send.at[phase, g, j], g_recv.at[phase, g], (lax.rem(row + j, PIECES), col))

    for phase in range(3):
        for g in range(GROUPS):
            stage_x(phase, g)
        for g in range(GROUPS):
            stage_relay(phase, g)
        if phase == 0:
            loads[2].wait()
            prepare(density, density_high, density_low)
        for g in range(GROUPS):
            stage_z(phase, g)
        for g in range(GROUPS):
            stage_gather(phase, g)

    parts = []
    for g in range(GROUPS):
        landed(gathered.at[2, g, pl.ds(0, 7)], g_recv.at[2, g])
        parts.append(gathered[2, g])
    for j in range(2):
        turned = [part[:, j * 8 : (j + 1) * 8].reshape(PIECES * 8, COLS) for part in parts]
        out[j] = jnp.concatenate(turned, axis=0).T
    for wait_send in sends:
        wait_send()


def step(fock, density, probe):
    f32, bf16 = jnp.float32, jnp.bfloat16
    vmem, dma = pltpu.VMEM, pltpu.SemaphoreType.DMA
    each = (3, GROUPS)
    return pl.pallas_call(
        kernel,
        out_shape=jax.ShapeDtypeStruct(probe.shape, f32),
        in_specs=[pl.BlockSpec(memory_space=pl.ANY)] * 3,
        out_specs=pl.BlockSpec(memory_space=pltpu.VMEM),
        scratch_shapes=[
            vmem(fock.shape, f32), vmem(density.shape, f32), vmem(probe.shape, f32),
            vmem((ROWS, 2 * COLS), bf16), vmem((ROWS, 2 * COLS), bf16),
            vmem((ROWS, 2 * COLS), bf16), vmem((ROWS, 2 * COLS), bf16),
            vmem((GROUPS, PIECES, DEPTH, COLS), f32),
            vmem((*each, 4, PIECES, DEPTH, COLS), f32),
            vmem((*each, 4, DEPTH, COLS), f32), vmem((*each, 4, DEPTH, COLS), f32),
            vmem((*each, PIECES, DEPTH, COLS), f32), vmem((*each, PIECES, DEPTH, COLS), f32),
            vmem((*each, PIECES, DEPTH, COLS), f32), vmem((*each, 8, DEPTH, COLS), f32),
            vmem((*each, PIECES, DEPTH, COLS), f32),
            dma((3,)), dma((*each, 6)), dma((*each, 6)), dma((*each, PIECES)), dma(each),
            dma((*each, PIECES)), dma(each),
        ],
        compiler_params=pltpu.CompilerParams(
            collective_id=0, has_side_effects=True, vmem_limit_bytes=40 * 1024 * 1024
        ),
    )(fock, density, probe)


def solution(mesh):
    return jax.shard_map(
        step,
        mesh=mesh,
        in_specs=(P(None, "row", "col"), P(None, "row", "col"), P(None, "col", None)),
        out_specs=P(None, "col", None),
        check_vma=False,
    )
```

```python
import functools

import jax
import jax.numpy as jnp
from jax import lax
from jax.experimental import pallas as pl
from jax.experimental.pallas import tpu as pltpu
from jax.sharding import PartitionSpec as P

MESH = pl.DeviceIdType.MESH
DT = 0.5
GROUPS = 2
ROWS = 1024
COLS = 256
PIECES = 8
DEPTH = 16
WIDE = PIECES * DEPTH


def split(value):
    high = value.astype(jnp.bfloat16)
    return high, (value - high.astype(jnp.float32)).astype(jnp.bfloat16)


def prepare(matrix, high, low):
    def part(i, carry):
        rows = pl.ds(pl.multiple_of(i * COLS, COLS), COLS)
        for j in range(2):
            h, l = split(matrix[j, rows, :])
            high[rows, j * COLS : (j + 1) * COLS] = h
            low[rows, j * COLS : (j + 1) * COLS] = l
        return carry

    lax.fori_loop(0, ROWS // COLS, part, 0)


def factors(phase, vector):
    real, imag = vector[:, :8], vector[:, 8:]
    if phase == 1:
        first, second = (real, imag), (-imag, real)
    else:
        dt = DT if phase == 0 else -DT
        first, second = (-dt * imag, dt * real), (-dt * real, -dt * imag)
    first = jnp.concatenate(first, axis=1).reshape(WIDE, COLS)
    second = jnp.concatenate(second, axis=1).reshape(WIDE, COLS)
    return jnp.concatenate([first, second], axis=1)


def times(high, low, matrix_high, matrix_low):
    dot = functools.partial(
        lax.dot_general,
        dimension_numbers=(((1,), (1,)), ((), ())),
        preferred_element_type=jnp.float32,
    )
    return dot(high, matrix_high) + (dot(low, matrix_high) + dot(high, matrix_low))


def kernel(
    fock_hbm, density_hbm, probe_hbm, out,
    fock, density, probe, fock_high, fock_low, density_high, density_low,
    start, chunks, relay_a, relay_b, from_left, from_right, summed, turned, arrived, gathered,
    load_sem, x_send, x_recv, y_send, y_recv, z_send, z_recv, g_send, g_recv,
):
    row, col = lax.axis_index("row"), lax.axis_index("col")
    z, x = col // 4, lax.rem(col, 4)
    right = z * 4 + lax.rem(x + 1, 4)
    left = z * 4 + lax.rem(x + 3, 4)
    y, core = row // 2, lax.rem(row, 2)

    def peer(dy, dc):
        return lax.rem(y + dy, 4) * 2 + lax.rem(core + dc, 2)

    peers = [peer(*d) for d in ((2, 0), (2, 1), (1, 0), (3, 0), (1, 1), (3, 1), (0, 1))]
    from_peers = [peer(*d) for d in ((0, 1), (1, 0), (3, 0), (1, 1), (3, 1), (2, 0), (2, 1))]

    loads = [
        pltpu.make_async_copy(source, target, load_sem.at[i])
        for i, (source, target) in enumerate(
            ((probe_hbm, probe), (fock_hbm, fock), (density_hbm, density))
        )
    ]
    for load in loads:
        load.start()

    barrier = pltpu.get_barrier_semaphore()

    def hello(r, c):
        pl.semaphore_signal(barrier, inc=1, device_id=(r, c), device_id_type=MESH)

    hello(row, right)
    hello(row, left)
    for j in range(1, PIECES):
        hello(lax.rem(row + j, PIECES), col)
        hello(row, lax.rem(z + j, 8) * 4 + x)

    loads[0].wait()
    for j in range(2):
        probe_t = probe[j].T
        for g in range(GROUPS):
            start[g, :, j * 8 : (j + 1) * 8, :] = probe_t[g * 64 : (g + 1) * 64].reshape(PIECES, 8, COLS)
    loads[1].wait()
    prepare(fock, fock_high, fock_low)

    sends = []

    def send(source, target, send_sem, recv_sem, device):
        copy = pltpu.make_async_remote_copy(
            src_ref=source, dst_ref=target, send_sem=send_sem, recv_sem=recv_sem,
            device_id=device, device_id_type=MESH,
        )
        copy.start()
        sends.append(copy.wait_send)

    def landing(target, sem):
        return pltpu.make_async_copy(target, target, sem).wait

    def landed(target, sem):
        landing(target, sem)()

    A, B = pl.ds(0, 4), pl.ds(4, 4)

    def multiply(phase, g):
        if phase == 0:
            vector = start[g]
        else:
            landed(gathered.at[phase - 1, g, pl.ds(0, 7)], g_recv.at[phase - 1, g])
            vector = gathered[phase - 1, g]
        high, low = split(factors(phase, vector))
        mh, ml = (density_high, density_low) if phase == 1 else (fock_high, fock_low)
        box = chunks.at[phase, g]

        def one(slot, ahead):
            rows = pl.ds(pl.multiple_of(lax.rem(x + ahead, 4) * COLS, COLS), COLS)
            box[slot] = times(high, low, mh[rows, :], ml[rows, :]).reshape(PIECES, DEPTH, COLS)

        return box, one

    def x_ends(phase, g):
        s, r = x_send.at[phase, g], x_recv.at[phase, g]
        return s, r

    def stage_x(phase, g):
        box, one = multiply(phase, g)
        s, r = x_ends(phase, g)
        one(0, 2)
        if phase == 0 and g == 0:
            pl.semaphore_wait(barrier, 16)

        send(box.at[0, A], relay_a.at[phase, g], s.at[0], r.at[0], (row, right))
        send(box.at[0, B], relay_b.at[phase, g], s.at[1], r.at[1], (row, left))
        one(1, 1)
        send(box.at[1, B], from_left.at[phase, g, B], s.at[2], r.at[2], (row, right))
        one(2, 3)
        send(box.at[2, A], from_right.at[phase, g, A], s.at[3], r.at[3], (row, left))
        one(3, 0)

    def stage_relay(phase, g):
        box = chunks.at[phase, g]
        s, r = x_ends(phase, g)
        landed(relay_a.at[phase, g], r.at[0])
        box[1, 0:4] = box[1, 0:4] + relay_a[phase, g]
        send(box.at[1, A], from_left.at[phase, g, A], s.at[4], r.at[4], (row, right))
        landed(relay_b.at[phase, g], r.at[1])
        box[2, 4:8] = box[2, 4:8] + relay_b[phase, g]
        send(box.at[2, B], from_right.at[phase, g, B], s.at[5], r.at[5], (row, left))

    def stage_y(phase, g):
        s, r = x_ends(phase, g)
        landed(from_left.at[phase, g, B], r.at[2])
        landed(from_right.at[phase, g, A], r.at[3])
        landed(from_left.at[phase, g, A], r.at[4])
        landed(from_right.at[phase, g, B], r.at[5])
        summed[phase, g] = chunks[phase, g, 3] + from_left[phase, g] + from_right[phase, g]
        s, r = y_send.at[phase, g], y_recv.at[phase, g]
        for p in peers:
            send(summed.at[phase, g, p], turned.at[phase, g, row], s.at[p], r.at[row], (p, col))
        along_z(phase, g, row, summed.at[phase, g, row])

    def along_z(phase, g, block, source):
        @pl.when(block != z)
        def _():
            pltpu.make_async_remote_copy(
                src_ref=source, dst_ref=arrived.at[phase, g, z],
                send_sem=z_send.at[phase, g, block], recv_sem=z_recv.at[phase, g],
                device_id=(row, block * 4 + x), device_id_type=MESH,
            ).start()

        @pl.when(block == z)
        def _():
            arrived[phase, g, z] = source[...]

    def stage_z(phase, g):
        for p in from_peers:
            piece = turned.at[phase, g, p]
            landed(piece, y_recv.at[phase, g, p])
            along_z(phase, g, p, piece)
        for j in range(1, 8):
            sends.append(landing(arrived.at[phase, g, 0], z_send.at[phase, g, lax.rem(z + j, 8)]))

    def stage_gather(phase, g):
        a = arrived.at[phase, g]
        landed(arrived.at[phase, g, pl.ds(0, 7)], z_recv.at[phase, g])
        total = ((a[0] + a[1]) + (a[2] + a[3])) + ((a[4] + a[5]) + (a[6] + a[7]))
        if phase == 0:
            total = total + start[g, row]
        if phase == 2:
            total = total + gathered[1, g, row]
        mine = gathered.at[phase, g, row]
        mine[...] = total
        for p in peers:
            send(mine, mine, g_send.at[phase, g, p], g_recv.at[phase, g], (p, col))

    for phase in range(3):
        for g in range(GROUPS):
            stage_x(phase, g)
        for g in range(GROUPS):
            stage_relay(phase, g)
        if phase == 0:
            loads[2].wait()
            prepare(density, density_high, density_low)
        for g in range(GROUPS):
            stage_y(phase, g)
        for g in range(GROUPS):
            stage_z(phase, g)
        for g in range(GROUPS):
            stage_gather(phase, g)

    parts = []
    for g in range(GROUPS):
        landed(gathered.at[2, g, pl.ds(0, 7)], g_recv.at[2, g])
        parts.append(gathered[2, g])
    for j in range(2):
        halves = [part[:, j * 8 : (j + 1) * 8].reshape(PIECES * 8, COLS) for part in parts]
        out[j] = jnp.concatenate(halves, axis=0).T
    for wait_send in sends:
        wait_send()


def step(fock, density, probe):
    f32, bf16 = jnp.float32, jnp.bfloat16
    vmem, dma = pltpu.VMEM, pltpu.SemaphoreType.DMA
    each = (3, GROUPS)
    return pl.pallas_call(
        kernel,
        out_shape=jax.ShapeDtypeStruct(probe.shape, f32),
        in_specs=[pl.BlockSpec(memory_space=pl.ANY)] * 3,
        out_specs=pl.BlockSpec(memory_space=pltpu.VMEM),
        scratch_shapes=[
            vmem(fock.shape, f32), vmem(density.shape, f32), vmem(probe.shape, f32),
            vmem((ROWS, 2 * COLS), bf16), vmem((ROWS, 2 * COLS), bf16),
            vmem((ROWS, 2 * COLS), bf16), vmem((ROWS, 2 * COLS), bf16),
            vmem((GROUPS, PIECES, DEPTH, COLS), f32),
            vmem((*each, 4, PIECES, DEPTH, COLS), f32),
            vmem((*each, 4, DEPTH, COLS), f32), vmem((*each, 4, DEPTH, COLS), f32),
            vmem((*each, PIECES, DEPTH, COLS), f32), vmem((*each, PIECES, DEPTH, COLS), f32),
            vmem((*each, PIECES, DEPTH, COLS), f32), vmem((*each, PIECES, DEPTH, COLS), f32),
            vmem((*each, 8, DEPTH, COLS), f32),
            vmem((*each, PIECES, DEPTH, COLS), f32),
            dma((3,)), dma((*each, 6)), dma((*each, 6)), dma((*each, PIECES)), dma((*each, PIECES)),
            dma((*each, 8)), dma(each),
            dma((*each, PIECES)), dma(each),
        ],
        compiler_params=pltpu.CompilerParams(
            collective_id=0, has_side_effects=True, vmem_limit_bytes=40 * 1024 * 1024
        ),
    )(fock, density, probe)


def solution(mesh):
    return jax.shard_map(
        step,
        mesh=mesh,
        in_specs=(P(None, "row", "col"), P(None, "row", "col"), P(None, "col", None)),
        out_specs=P(None, "col", None),
        check_vma=False,
    )
```

```python
import functools

import jax
import jax.numpy as jnp
from jax import lax
from jax.experimental import pallas as pl
from jax.experimental.pallas import tpu as pltpu
from jax.sharding import PartitionSpec as P

MESH = pl.DeviceIdType.MESH
DT = 0.5
ROWS = 1024
COLS = 256
PIECES = 8
DEPTH = 16
GROUPS = 2
CUTS = GROUPS // 2
WIDE = COLS // CUTS
KINDS = PIECES // CUTS
TALL = KINDS * DEPTH
PHASES = 3
TIMES = {"x": 0.0, "relay": 3.1, "y": 6.2, "z": 10.0, "gather": 16.0}
PERIOD = 21.0
APART = 4.2


def timetable():
    turns = [
        (phase * PERIOD + g * APART + at, phase, g, name)
        for phase in range(PHASES)
        for g in range(GROUPS)
        for name, at in TIMES.items()
    ]
    return [turn[1:] for turn in sorted(turns, key=lambda turn: turn[0])]


def split(value):
    high = value.astype(jnp.bfloat16)
    return high, (value - high.astype(jnp.float32)).astype(jnp.bfloat16)


def prepare(matrix, high, low):
    def part(i, carry):
        rows = pl.ds(pl.multiple_of(i * COLS, COLS), COLS)
        for j in range(2):
            h, l = split(matrix[j, rows, :])
            high[rows, j * COLS : (j + 1) * COLS] = h
            low[rows, j * COLS : (j + 1) * COLS] = l
        return carry

    lax.fori_loop(0, ROWS // COLS, part, 0)


def flat(vector):
    parts = [vector[i * KINDS : (i + 1) * KINDS].reshape(TALL, WIDE) for i in range(CUTS)]
    return jnp.concatenate(parts, axis=1) if CUTS > 1 else parts[0]


def factors(phase, vector):
    real, imag = vector[:, :8], vector[:, 8:]
    if phase == 1:
        first, second = (real, imag), (-imag, real)
    else:
        dt = DT if phase == 0 else -DT
        first, second = (-dt * imag, dt * real), (-dt * real, -dt * imag)
    first = flat(jnp.concatenate(first, axis=1))
    second = flat(jnp.concatenate(second, axis=1))
    return jnp.concatenate([first, second], axis=1)


def times(high, low, matrix_high, matrix_low):
    dot = functools.partial(
        lax.dot_general,
        dimension_numbers=(((1,), (1,)), ((), ())),
        preferred_element_type=jnp.float32,
    )
    both = dot(jnp.concatenate([high, low], axis=0), matrix_high)
    return both[:TALL] + (both[TALL:] + dot(high, matrix_low))


def kernel(
    fock_hbm, density_hbm, probe_hbm, out,
    fock, density, probe, fock_high, fock_low, density_high, density_low,
    start, chunks, relay_a, relay_b, from_left, from_right, summed, turned, arrived, gathered,
    load_sem, x_send, x_recv, y_send, y_recv, z_send, z_recv, g_send, g_recv,
):
    row, col = lax.axis_index("row"), lax.axis_index("col")
    z, x = col // 4, lax.rem(col, 4)
    right = z * 4 + lax.rem(x + 1, 4)
    left = z * 4 + lax.rem(x + 3, 4)
    y, core = row // 2, lax.rem(row, 2)

    def peer(dy, dc):
        return lax.rem(y + dy, 4) * 2 + lax.rem(core + dc, 2)

    peers = [peer(*d) for d in ((2, 0), (2, 1), (1, 0), (3, 0), (1, 1), (3, 1), (0, 1))]
    from_peers = [peer(*d) for d in ((0, 1), (1, 0), (3, 0), (1, 1), (3, 1), (2, 0), (2, 1))]

    loads = [
        pltpu.make_async_copy(source, target, load_sem.at[i])
        for i, (source, target) in enumerate(
            ((probe_hbm, probe), (fock_hbm, fock), (density_hbm, density))
        )
    ]
    for load in loads:
        load.start()

    barrier = pltpu.get_barrier_semaphore()

    def hello(r, c):
        pl.semaphore_signal(barrier, inc=1, device_id=(r, c), device_id_type=MESH)

    for j in range(1, 8):
        hello(row, lax.rem(z + j, 8) * 4 + x)
    for p in peers:
        hello(p, col)
    hello(row, right)
    hello(row, left)

    loads[0].wait()
    for j in range(2):
        probe_t = probe[j].T.reshape(GROUPS, KINDS, 8, COLS)
        for i in range(CUTS):
            start[:, i * KINDS : (i + 1) * KINDS, j * 8 : (j + 1) * 8, :] = probe_t[..., i * WIDE : (i + 1) * WIDE]
    loads[1].wait()
    prepare(fock, fock_high, fock_low)

    sends = []

    def send(source, target, send_sem, recv_sem, device):
        copy = pltpu.make_async_remote_copy(
            src_ref=source, dst_ref=target, send_sem=send_sem, recv_sem=recv_sem,
            device_id=device, device_id_type=MESH,
        )
        copy.start()
        sends.append(copy.wait_send)

    def landing(target, sem):
        return pltpu.make_async_copy(target, target, sem).wait

    def landed(target, sem):
        landing(target, sem)()

    A, B = pl.ds(0, 4), pl.ds(4, 4)

    def stage_x(phase, g):
        if phase == 0:
            vector = start[g]
        else:
            landed(gathered.at[phase - 1, g, pl.ds(0, 7)], g_recv.at[phase - 1, g])
            vector = gathered[phase - 1, g]
        high, low = split(factors(phase, vector))
        mh, ml = (density_high, density_low) if phase == 1 else (fock_high, fock_low)
        box = chunks.at[phase, g]
        s, r = x_send.at[phase, g], x_recv.at[phase, g]

        def one(slot, ahead):
            rows = pl.ds(pl.multiple_of(lax.rem(x + ahead, 4) * COLS, COLS), COLS)
            value = times(high, low, mh[rows, :], ml[rows, :])
            for i in range(CUTS):
                box[slot, i * KINDS : (i + 1) * KINDS] = value[:, i * WIDE : (i + 1) * WIDE].reshape(KINDS, DEPTH, WIDE)

        one(0, 2)
        if phase == 0 and g == 0:
            pl.semaphore_wait(barrier, 16)
        send(box.at[0, A], relay_a.at[phase, g], s.at[0], r.at[0], (row, right))
        send(box.at[0, B], relay_b.at[phase, g], s.at[1], r.at[1], (row, left))
        one(1, 1)
        send(box.at[1, B], from_left.at[phase, g, B], s.at[2], r.at[2], (row, right))
        one(2, 3)
        send(box.at[2, A], from_right.at[phase, g, A], s.at[3], r.at[3], (row, left))
        one(3, 0)

    def stage_relay(phase, g):
        box = chunks.at[phase, g]
        s, r = x_send.at[phase, g], x_recv.at[phase, g]
        landed(relay_a.at[phase, g], r.at[0])
        box[1, 0:4] = box[1, 0:4] + relay_a[phase, g]
        send(box.at[1, A], from_left.at[phase, g, A], s.at[4], r.at[4], (row, right))
        landed(relay_b.at[phase, g], r.at[1])
        box[2, 4:8] = box[2, 4:8] + relay_b[phase, g]
        send(box.at[2, B], from_right.at[phase, g, B], s.at[5], r.at[5], (row, left))

    def stage_y(phase, g):
        r = x_recv.at[phase, g]
        landed(from_left.at[phase, g, B], r.at[2])
        landed(from_right.at[phase, g, A], r.at[3])
        landed(from_left.at[phase, g, A], r.at[4])
        landed(from_right.at[phase, g, B], r.at[5])
        summed[phase, g] = chunks[phase, g, 3] + from_left[phase, g] + from_right[phase, g]
        s, r = y_send.at[phase, g], y_recv.at[phase, g]
        for p in peers:
            send(summed.at[phase, g, p], turned.at[phase, g, row], s.at[p], r.at[row], (p, col))
        turned[phase, g, row] = summed[phase, g, row]
        along_z(phase, g, row, summed.at[phase, g, row])

    def along_z(phase, g, block, source):
        @pl.when(block != z)
        def _():
            pltpu.make_async_remote_copy(
                src_ref=source, dst_ref=arrived.at[phase, g, z],
                send_sem=z_send.at[phase, g, block], recv_sem=z_recv.at[phase, g],
                device_id=(row, block * 4 + x), device_id_type=MESH,
            ).start()

    def stage_z(phase, g):
        for p in from_peers:
            piece = turned.at[phase, g, p]
            landed(piece, y_recv.at[phase, g, p])
            along_z(phase, g, p, piece)
        arrived[phase, g, z] = turned[phase, g, z]
        for j in range(1, 8):
            sends.append(landing(arrived.at[phase, g, 0], z_send.at[phase, g, lax.rem(z + j, 8)]))

    def stage_gather(phase, g):
        a = arrived.at[phase, g]
        landed(arrived.at[phase, g, pl.ds(0, 7)], z_recv.at[phase, g])
        total = ((a[0] + a[1]) + (a[2] + a[3])) + ((a[4] + a[5]) + (a[6] + a[7]))
        if phase == 0:
            total = total + start[g, row]
        if phase == 2:
            total = total + gathered[1, g, row]
        mine = gathered.at[phase, g, row]
        mine[...] = total
        for p in peers:
            send(mine, mine, g_send.at[phase, g, p], g_recv.at[phase, g], (p, col))

    stages = {"x": stage_x, "relay": stage_relay, "y": stage_y, "z": stage_z, "gather": stage_gather}
    ready = False
    for phase, g, name in timetable():
        if phase == 0 and name == "y" and not ready:
            ready = True
            loads[2].wait()
            prepare(density, density_high, density_low)
        stages[name](phase, g)

    parts = []
    for g in range(GROUPS):
        landed(gathered.at[2, g, pl.ds(0, 7)], g_recv.at[2, g])
        parts.append(gathered[2, g])
    for j in range(2):
        halves = []
        for part in parts:
            half = part[:, j * 8 : (j + 1) * 8]
            cuts = [half[i * KINDS : (i + 1) * KINDS].reshape(KINDS * 8, WIDE) for i in range(CUTS)]
            halves.append(jnp.concatenate(cuts, axis=1) if CUTS > 1 else cuts[0])
        out[j] = jnp.concatenate(halves, axis=0).T
    for wait_send in sends:
        wait_send()


def step(fock, density, probe):
    f32, bf16 = jnp.float32, jnp.bfloat16
    vmem, dma = pltpu.VMEM, pltpu.SemaphoreType.DMA
    each = (PHASES, GROUPS)
    piece = (DEPTH, WIDE)
    return pl.pallas_call(
        kernel,
        out_shape=jax.ShapeDtypeStruct(probe.shape, f32),
        in_specs=[pl.BlockSpec(memory_space=pltpu.HBM)] * 3,
        out_specs=pl.BlockSpec(memory_space=pltpu.VMEM),
        scratch_shapes=[
            vmem(fock.shape, f32), vmem(density.shape, f32), vmem(probe.shape, f32),
            vmem((ROWS, 2 * COLS), bf16), vmem((ROWS, 2 * COLS), bf16),
            vmem((ROWS, 2 * COLS), bf16), vmem((ROWS, 2 * COLS), bf16),
            vmem((GROUPS, PIECES, *piece), f32),
            vmem((*each, 4, PIECES, *piece), f32),
            vmem((*each, 4, *piece), f32), vmem((*each, 4, *piece), f32),
            vmem((*each, PIECES, *piece), f32), vmem((*each, PIECES, *piece), f32),
            vmem((*each, PIECES, *piece), f32), vmem((*each, PIECES, *piece), f32),
            vmem((*each, 8, *piece), f32), vmem((*each, PIECES, *piece), f32),
            dma((3,)), dma((*each, 6)), dma((*each, 6)), dma((*each, PIECES)), dma((*each, PIECES)),
            dma((*each, 8)), dma(each), dma((*each, PIECES)), dma(each),
        ],
        compiler_params=pltpu.CompilerParams(
            collective_id=0, has_side_effects=True, vmem_limit_bytes=60 * 1024 * 1024
        ),
    )(fock, density, probe)


def solution(mesh):
    return jax.shard_map(
        step,
        mesh=mesh,
        in_specs=(P(None, "row", "col"), P(None, "row", "col"), P(None, "col", None)),
        out_specs=P(None, "col", None),
        check_vma=False,
    )
```

```python
import functools

import jax
import jax.numpy as jnp
from jax import lax
from jax.experimental import pallas as pl
from jax.experimental.pallas import tpu as pltpu
from jax.sharding import PartitionSpec as P

MESH = pl.DeviceIdType.MESH
DT = 0.5
ROWS = 1024
COLS = 256
PIECES = 8
DEPTH = 16
GROUPS = 2
CUTS = GROUPS // 2
WIDE = COLS // CUTS
KINDS = PIECES // CUTS
TALL = KINDS * DEPTH
PHASES = 3
VMEM_LIMIT = 60 * 1024 * 1024
APART = 4.2


def split(value):
    high = value.astype(jnp.bfloat16)
    return high, (value - high.astype(jnp.float32)).astype(jnp.bfloat16)


def flat(vector):
    parts = [vector[i * KINDS : (i + 1) * KINDS].reshape(TALL, WIDE) for i in range(CUTS)]
    return jnp.concatenate(parts, axis=1) if CUTS > 1 else parts[0]


def factors(phase, vector):
    real, imag = vector[:, :8], vector[:, 8:]
    if phase == 1:
        first, second = (real, imag), (imag, -real)
    else:
        dt = DT if phase == 0 else -DT
        first, second = (-dt * imag, dt * real), (-dt * real, -dt * imag)
    first = flat(jnp.concatenate(first, axis=1))
    second = flat(jnp.concatenate(second, axis=1))
    return split(jnp.concatenate([first, second], axis=1))


def times(high, low, matrix_high, matrix_low, depth_dim):
    dot = functools.partial(
        lax.dot_general,
        dimension_numbers=(((1,), (depth_dim,)), ((), ())),
        preferred_element_type=jnp.float32,
    )
    both = dot(jnp.concatenate([high, low], axis=0), matrix_high)
    return both[:TALL] + (both[TALL:] + dot(high, matrix_low))


def kernel(
    fock_hbm, density_hbm, probe_hbm, out,
    fock, density, probe, fock_high, fock_low, density_high, density_low,
    start, chunks, relay_a, relay_b, from_left, from_right, summed, turned, arrived, blocks, sums, gathered,
    load_sem, x_send, x_recv, y_send, y_recv, z_send, z_recv, g_send, g_recv, zg_send, zg_recv, xg_send, xg_recv,
):
    row, col = lax.axis_index("row"), lax.axis_index("col")
    z, x = col // 4, lax.rem(col, 4)
    y, core = row // 2, lax.rem(row, 2)
    right = (row, z * 4 + lax.rem(x + 1, 4))
    left = (row, z * 4 + lax.rem(x + 3, 4))

    def along_x(ahead):
        return lax.rem(x + ahead, 4)

    def along_z(ahead):
        return lax.rem(z + ahead, 8)

    def peer(dy, dc):
        return lax.rem(y + dy, 4) * 2 + lax.rem(core + dc, 2)

    peers = [peer(*d) for d in ((2, 0), (2, 1), (1, 0), (3, 0), (1, 1), (3, 1), (0, 1))]
    from_peers = [peer(*d) for d in ((0, 1), (1, 0), (3, 0), (1, 1), (3, 1), (2, 0), (2, 1))]
    z_order = (4, 3, 5, 2, 6, 1, 7)

    barrier = pltpu.get_barrier_semaphore()

    def hello(r, c):
        pl.semaphore_signal(barrier, inc=1, device_id=(r, c), device_id_type=MESH)

    for j in z_order:
        hello(row, along_z(j) * 4 + x)
    for p in peers:
        hello(p, col)
    hello(*right)
    hello(*left)

    def rows_of(block):
        return pl.ds(pl.multiple_of(block * COLS, COLS), COLS)

    probe_load = pltpu.make_async_copy(probe_hbm, probe, load_sem.at[0])
    density_load = pltpu.make_async_copy(density_hbm, density, load_sem.at[1])
    fock_loads = {}
    probe_load.start()
    for i, ahead in enumerate((2, 1, 3, 0)):
        rows = rows_of(along_x(ahead))
        fock_loads[ahead] = pltpu.make_async_copy(fock_hbm.at[:, rows, :], fock.at[:, rows, :], load_sem.at[2 + i])
        fock_loads[ahead].start()

    probe_load.wait()
    for j in range(2):
        probe_t = probe[j].T.reshape(GROUPS, KINDS, 8, COLS)
        for i in range(CUTS):
            start[:, i * KINDS : (i + 1) * KINDS, j * 8 : (j + 1) * 8, :] = probe_t[..., i * WIDE : (i + 1) * WIDE]

    sends = []

    def send(source, target, send_sem, recv_sem, device):
        copy = pltpu.make_async_remote_copy(
            src_ref=source, dst_ref=target, send_sem=send_sem, recv_sem=recv_sem,
            device_id=device, device_id_type=MESH,
        )
        copy.start()
        sends.append(copy.wait_send)

    def landing(target, sem):
        return pltpu.make_async_copy(target, target, sem).wait

    def landed(target, sem):
        landing(target, sem)()

    def store(box, value):
        for i in range(CUTS):
            box[i * KINDS : (i + 1) * KINDS] = value[:, i * WIDE : (i + 1) * WIDE].reshape(KINDS, DEPTH, WIDE)

    A, B = pl.ds(0, 4), pl.ds(4, 4)

    def stage_x(phase, g):
        if phase == 0:
            vector = start[g]
        else:
            landed(gathered.at[1, g, pl.ds(0, 7)], g_recv.at[1, g])
            vector = gathered[1, g]
        high, low = factors(phase, vector)
        box = chunks.at[phase, g]
        s, r = x_send.at[phase, g], x_recv.at[phase, g]

        def one(slot, ahead):
            rows = rows_of(along_x(ahead))
            if phase == 0 and g == 0:
                fock_loads[ahead].wait()
                for j in range(2):
                    h, l = split(fock[j, rows, :])
                    fock_high[rows, j * COLS : (j + 1) * COLS] = h
                    fock_low[rows, j * COLS : (j + 1) * COLS] = l
            store(box.at[slot], times(high, low, fock_high[rows, :], fock_low[rows, :], 1))

        one(0, 2)
        if phase == 0 and g == 0:
            pl.semaphore_wait(barrier, 16)
        send(box.at[0, A], relay_a.at[phase, g], s.at[0], r.at[0], right)
        send(box.at[0, B], relay_b.at[phase, g], s.at[1], r.at[1], left)
        one(1, 1)
        send(box.at[1, B], from_left.at[phase, g, B], s.at[2], r.at[2], right)
        one(2, 3)
        send(box.at[2, A], from_right.at[phase, g, A], s.at[3], r.at[3], left)
        one(3, 0)
        if phase == 0:
            if g == 0:
                density_load.start()

            @pl.when(z == row)
            def _():
                box[3] = box[3] + start[g]

    def stage_relay(phase, g):
        box = chunks.at[phase, g]
        s, r = x_send.at[phase, g], x_recv.at[phase, g]
        landed(relay_a.at[phase, g], r.at[0])
        box[1, 0:4] = box[1, 0:4] + relay_a[phase, g]
        send(box.at[1, A], from_left.at[phase, g, A], s.at[4], r.at[4], right)
        landed(relay_b.at[phase, g], r.at[1])
        box[2, 4:8] = box[2, 4:8] + relay_b[phase, g]
        send(box.at[2, B], from_right.at[phase, g, B], s.at[5], r.at[5], left)

    def sum_x(phase, g):
        r = x_recv.at[phase, g]
        landed(from_left.at[phase, g, B], r.at[2])
        landed(from_right.at[phase, g, A], r.at[3])
        landed(from_left.at[phase, g, A], r.at[4])
        landed(from_right.at[phase, g, B], r.at[5])
        summed[phase, g] = chunks[phase, g, 3] + from_left[phase, g] + from_right[phase, g]

    def sum_of(a):
        return ((a[0] + a[1]) + (a[2] + a[3])) + ((a[4] + a[5]) + (a[6] + a[7]))

    def stage_spread(g):
        sum_x(0, g)
        for o in z_order:
            j = along_z(o)
            send(summed.at[0, g, j], arrived.at[0, g, z], z_send.at[0, g, j], z_recv.at[0, g], (row, j * 4 + x))
        arrived[0, g, z] = summed[0, g, z]

    def stage_collect(g):
        landed(arrived.at[0, g, pl.ds(0, 7)], z_recv.at[0, g])
        mine = blocks.at[g, x, z]
        mine[...] = sum_of(arrived.at[0, g])
        for o in z_order:
            j = along_z(o)
            send(mine, mine, zg_send.at[g, j], zg_recv.at[g, z], (row, j * 4 + x))
        forward(g, 0)

    def forward(g, *offsets):
        for o in offsets:
            j = along_z(o)
            piece = blocks.at[g, x, j]
            if o:
                landed(piece, zg_recv.at[g, j])
            send(piece, piece, xg_send.at[g, 0, j], xg_recv.at[g, 0, j], right)
            send(piece, piece, xg_send.at[g, 1, j], xg_recv.at[g, 1, j], left)

    def onward(g, *offsets):
        for o in offsets:
            j = along_z(o)
            back, at, way = (3, 0, right) if o < 4 else (1, 1, left)
            piece = blocks.at[g, along_x(back), j]
            landed(piece, xg_recv.at[g, at, j])
            send(piece, piece, xg_send.at[g, 2, j], xg_recv.at[g, 2, j], way)

    def adjoint(g, ahead):
        block = along_x(ahead)
        high, low = factors(1, blocks[g, block])
        return times(high, low, density_high[block], density_low[block], 0)

    def stage_own(g):
        sums[g] = adjoint(g, 0)

    def stage_next(g):
        for o in range(8):
            j = along_z(o)
            back, at = (1, 1) if o < 4 else (3, 0)
            landed(blocks.at[g, along_x(back), j], xg_recv.at[g, at, j])
        sums[g] = sums[g] + (adjoint(g, 1) + adjoint(g, 3))

    def stage_far(g):
        for o in range(8):
            j = along_z(o)
            landed(blocks.at[g, along_x(2), j], xg_recv.at[g, 2, j])
        store(summed.at[1, g], sums[g] + adjoint(g, 2))
        for p in peers:
            send(summed.at[1, g, p], turned.at[1, g, row], y_send.at[1, g, p], y_recv.at[1, g, 0], (p, col))
        turned[1, g, row] = summed[1, g, row]

    def stage_join(g):
        landed(turned.at[1, g, pl.ds(0, 7)], y_recv.at[1, g, 0])
        gather(1, g, sum_of(turned.at[1, g]))

    def gather(phase, g, value):
        mine = gathered.at[phase, g, row]
        mine[...] = value
        for p in peers:
            send(mine, mine, g_send.at[phase, g, p], g_recv.at[phase, g], (p, col))

    def to_z(g, block, source):
        @pl.when(block != z)
        def _():
            pltpu.make_async_remote_copy(
                src_ref=source, dst_ref=arrived.at[2, g, z],
                send_sem=z_send.at[2, g, block], recv_sem=z_recv.at[2, g],
                device_id=(row, block * 4 + x), device_id_type=MESH,
            ).start()

    def stage_y(g):
        sum_x(2, g)
        for p in peers:
            send(summed.at[2, g, p], turned.at[2, g, row], y_send.at[2, g, p], y_recv.at[2, g, row], (p, col))
        turned[2, g, row] = summed[2, g, row]
        to_z(g, row, summed.at[2, g, row])

    def stage_z(g):
        for p in from_peers:
            piece = turned.at[2, g, p]
            landed(piece, y_recv.at[2, g, p])
            to_z(g, p, piece)
        arrived[2, g, z] = turned[2, g, z]
        for j in range(1, 8):
            sends.append(landing(arrived.at[2, g, 0], z_send.at[2, g, along_z(j)]))

    def stage_gather(g):
        landed(arrived.at[2, g, pl.ds(0, 7)], z_recv.at[2, g])
        gather(2, g, sum_of(arrived.at[2, g]) + gathered[1, g, row])

    def stage_density(g):
        if g == 0:
            density_load.wait()

            def part(i, carry):
                for j in range(2):
                    h, l = split(density[j, rows_of(i), :])
                    density_high[i, j * COLS : (j + 1) * COLS] = h
                    density_low[i, j * COLS : (j + 1) * COLS] = l
                return carry

            lax.fori_loop(0, ROWS // COLS, part, 0)

    def stage_out(g):
        landed(gathered.at[2, g, pl.ds(0, 7)], g_recv.at[2, g])
        part, each = gathered[2, g], KINDS * 8
        for j in range(2):
            half = part[:, j * 8 : (j + 1) * 8]
            cuts = [half[i * KINDS : (i + 1) * KINDS].reshape(each, WIDE) for i in range(CUTS)]
            whole = jnp.concatenate(cuts, axis=1) if CUTS > 1 else cuts[0]
            out[j, :, g * each : (g + 1) * each] = whole.T

    plan = (
        (0.0, functools.partial(stage_x, 0)),
        (4.0, functools.partial(stage_relay, 0)),
        (5.0, stage_density),
        (7.3, stage_spread),
        (12.6, stage_collect),
        (15.4, lambda g: forward(g, 1, 7)),
        (15.5, lambda g: onward(g, 0)),
        (16.2, lambda g: forward(g, 2, 6)),
        (17.0, lambda g: forward(g, 3, 5)),
        (17.8, lambda g: forward(g, 4)),
        (18.2, lambda g: onward(g, 1, 7)),
        (18.3, stage_own),
        (19.0, lambda g: onward(g, 2, 6)),
        (19.8, lambda g: onward(g, 3, 5)),
        (20.6, lambda g: onward(g, 4)),
        (20.7, stage_next),
        (23.5, stage_far),
        (28.5, stage_join),
        (33.0, functools.partial(stage_x, 2)),
        (37.5, functools.partial(stage_relay, 2)),
        (40.8, stage_y),
        (45.6, stage_z),
        (51.0, stage_gather),
        (55.5, stage_out),
    )
    turns = [(at + g * APART, g, stage) for at, stage in plan for g in range(GROUPS)]
    for _, g, stage in sorted(turns, key=lambda turn: turn[0]):
        stage(g)
    for wait_send in sends:
        wait_send()


def step(fock, density, probe):
    f32, bf16 = jnp.float32, jnp.bfloat16
    vmem, dma = pltpu.VMEM, pltpu.SemaphoreType.DMA
    each = (PHASES, GROUPS)
    piece = (DEPTH, WIDE)
    return pl.pallas_call(
        kernel,
        out_shape=jax.ShapeDtypeStruct(probe.shape, f32),
        in_specs=[pl.BlockSpec(memory_space=pltpu.HBM)] * 3,
        out_specs=pl.BlockSpec(memory_space=pltpu.VMEM),
        scratch_shapes=[
            vmem(fock.shape, f32), vmem(density.shape, f32), vmem(probe.shape, f32),
            vmem((ROWS, 2 * COLS), bf16), vmem((ROWS, 2 * COLS), bf16),
            vmem((ROWS // COLS, 2 * COLS, COLS), bf16), vmem((ROWS // COLS, 2 * COLS, COLS), bf16),
            vmem((GROUPS, PIECES, *piece), f32),
            vmem((*each, 4, PIECES, *piece), f32),
            vmem((*each, 4, *piece), f32), vmem((*each, 4, *piece), f32),
            vmem((*each, PIECES, *piece), f32), vmem((*each, PIECES, *piece), f32),
            vmem((*each, PIECES, *piece), f32), vmem((*each, PIECES, *piece), f32),
            vmem((*each, 8, *piece), f32), vmem((GROUPS, 4, PIECES, *piece), f32),
            vmem((GROUPS, TALL, COLS), f32), vmem((*each, PIECES, *piece), f32),
            dma((6,)), dma((*each, 6)), dma((*each, 6)), dma((*each, PIECES)), dma((*each, PIECES)),
            dma((*each, 8)), dma(each), dma((*each, PIECES)), dma(each),
            dma((GROUPS, 8)), dma((GROUPS, 8)), dma((GROUPS, 3, 8)), dma((GROUPS, 3, 8)),
        ],
        compiler_params=pltpu.CompilerParams(
            collective_id=0, has_side_effects=True, vmem_limit_bytes=VMEM_LIMIT
        ),
    )(fock, density, probe)


def solution(mesh):
    return jax.shard_map(
        step,
        mesh=mesh,
        in_specs=(P(None, "row", "col"), P(None, "row", "col"), P(None, "col", None)),
        out_specs=P(None, "col", None),
        check_vma=False,
    )
```

```python
import functools

import jax
import jax.numpy as jnp
from jax import lax
from jax.experimental import pallas as pl
from jax.experimental.pallas import tpu as pltpu
from jax.sharding import PartitionSpec as P

MESH = pl.DeviceIdType.MESH
DT = 0.5
ROWS = 1024
COLS = 256
PIECES = 8
DEPTH = 16
GROUPS = 2
CUTS = GROUPS // 2
WIDE = COLS // CUTS
KINDS = PIECES // CUTS
TALL = KINDS * DEPTH
PHASES = 3
VMEM_LIMIT = 60 * 1024 * 1024
APART = 5.6


def split(value):
    high = value.astype(jnp.bfloat16)
    return high, (value - high.astype(jnp.float32)).astype(jnp.bfloat16)


def flat(vector):
    parts = [vector[i * KINDS : (i + 1) * KINDS].reshape(TALL, WIDE) for i in range(CUTS)]
    return jnp.concatenate(parts, axis=1) if CUTS > 1 else parts[0]


def factors(phase, vector):
    real, imag = vector[:, :8], vector[:, 8:]
    if phase == 1:
        first, second = (real, imag), (imag, -real)
    else:
        dt = DT if phase == 0 else -DT
        first, second = (-dt * imag, dt * real), (-dt * real, -dt * imag)
    first = flat(jnp.concatenate(first, axis=1))
    second = flat(jnp.concatenate(second, axis=1))
    return split(jnp.concatenate([first, second], axis=1))


def times(high, low, matrix_high, matrix_low, depth_dim):
    dot = functools.partial(
        lax.dot_general,
        dimension_numbers=(((1,), (depth_dim,)), ((), ())),
        preferred_element_type=jnp.float32,
    )
    both = dot(jnp.concatenate([high, low], axis=0), matrix_high)
    return both[:TALL] + (both[TALL:] + dot(high, matrix_low))


def kernel(
    fock_hbm, density_hbm, probe_hbm, out,
    fock, density, probe, fock_high, fock_low, density_high, density_low,
    start, chunks, relay_a, relay_b, from_left, from_right, summed, turned, arrived, blocks, sums, gathered,
    load_sem, x_send, x_recv, y_send, y_recv, z_send, z_recv, g_send, g_recv, zg_send, zg_recv, xg_send, xg_recv,
):
    row, col = lax.axis_index("row"), lax.axis_index("col")
    z, x = col // 4, lax.rem(col, 4)
    y, core = row // 2, lax.rem(row, 2)
    right = (row, z * 4 + lax.rem(x + 1, 4))
    left = (row, z * 4 + lax.rem(x + 3, 4))

    def along_x(ahead):
        return lax.rem(x + ahead, 4)

    def along_z(ahead):
        return lax.rem(z + ahead, 8)

    def peer(dy, dc):
        return lax.rem(y + dy, 4) * 2 + lax.rem(core + dc, 2)

    peers = [peer(*d) for d in ((2, 0), (2, 1), (1, 0), (3, 0), (1, 1), (3, 1), (0, 1))]
    from_peers = [peer(*d) for d in ((0, 1), (1, 0), (3, 0), (1, 1), (3, 1), (2, 0), (2, 1))]
    z_order = (4, 3, 5, 2, 6, 1, 7)

    barrier = pltpu.get_barrier_semaphore()

    def hello(r, c):
        pl.semaphore_signal(barrier, inc=1, device_id=(r, c), device_id_type=MESH)

    for j in z_order:
        hello(row, along_z(j) * 4 + x)
    for p in peers:
        hello(p, col)
    hello(*right)
    hello(*left)

    def rows_of(block):
        return pl.ds(pl.multiple_of(block * COLS, COLS), COLS)

    probe_load = pltpu.make_async_copy(probe_hbm, probe, load_sem.at[0])
    density_load = pltpu.make_async_copy(density_hbm, density, load_sem.at[1])
    fock_loads = {}
    probe_load.start()
    for i, ahead in enumerate((2, 1, 3, 0)):
        rows = rows_of(along_x(ahead))
        fock_loads[ahead] = pltpu.make_async_copy(fock_hbm.at[:, rows, :], fock.at[:, rows, :], load_sem.at[2 + i])
        fock_loads[ahead].start()

    probe_load.wait()
    for j in range(2):
        probe_t = probe[j].T.reshape(GROUPS, KINDS, 8, COLS)
        for i in range(CUTS):
            start[:, i * KINDS : (i + 1) * KINDS, j * 8 : (j + 1) * 8, :] = probe_t[..., i * WIDE : (i + 1) * WIDE]

    def send(source, target, send_sem, recv_sem, device):
        copy = pltpu.make_async_remote_copy(
            src_ref=source, dst_ref=target, send_sem=send_sem, recv_sem=recv_sem,
            device_id=device, device_id_type=MESH,
        )
        copy.start()

    def landed(target, sem):
        pltpu.make_async_copy(target, target, sem).wait()

    def store(box, value):
        for i in range(CUTS):
            box[i * KINDS : (i + 1) * KINDS] = value[:, i * WIDE : (i + 1) * WIDE].reshape(KINDS, DEPTH, WIDE)

    FIRST, LAST = pl.ds(0, 4), pl.ds(4, 4)
    A, B = (pl.ds(0, 2), pl.ds(2, 2)), (pl.ds(4, 2), pl.ds(6, 2))

    def stage_x(phase, g):
        if phase == 0:
            vector = start[g]
        else:
            landed(gathered.at[1, g, pl.ds(0, 7)], g_recv.at[1, g])
            vector = gathered[1, g]
        high, low = factors(phase, vector)
        box = chunks.at[phase, g]
        s, r = x_send.at[phase, g], x_recv.at[phase, g]

        def one(slot, ahead):
            rows = rows_of(along_x(ahead))
            if phase == 0 and g == 0:
                fock_loads[ahead].wait()
                for j in range(2):
                    h, l = split(fock[j, rows, :])
                    fock_high[rows, j * COLS : (j + 1) * COLS] = h
                    fock_low[rows, j * COLS : (j + 1) * COLS] = l
            store(box.at[slot], times(high, low, fock_high[rows, :], fock_low[rows, :], 1))

        one(0, 2)
        if phase == 0 and g == 0:
            pl.semaphore_wait(barrier, 16)
        for i in range(2):
            send(box.at[0, A[i]], relay_a.at[phase, g, i], s, r.at[i], right)
            send(box.at[0, B[i]], relay_b.at[phase, g, i], s, r.at[2 + i], left)
        one(1, 1)
        send(box.at[1, LAST], from_left.at[phase, g, LAST], s, r.at[4], right)
        one(2, 3)
        send(box.at[2, FIRST], from_right.at[phase, g, FIRST], s, r.at[5], left)
        one(3, 0)
        if phase == 0:
            if g == 0:
                density_load.start()

            @pl.when(z == row)
            def _():
                box[3] = box[3] + start[g]

    def stage_relay(phase, g):
        box = chunks.at[phase, g]
        s, r = x_send.at[phase, g], x_recv.at[phase, g]
        for i in range(2):
            landed(relay_a.at[phase, g, i], r.at[i])
            box[1, A[i]] = box[1, A[i]] + relay_a[phase, g, i]
            send(box.at[1, A[i]], from_left.at[phase, g, A[i]], s, r.at[6 + i], right)
            landed(relay_b.at[phase, g, i], r.at[2 + i])
            box[2, B[i]] = box[2, B[i]] + relay_b[phase, g, i]
            send(box.at[2, B[i]], from_right.at[phase, g, B[i]], s, r.at[8 + i], left)

    def sum_x(phase, g):
        r = x_recv.at[phase, g]
        landed(from_left.at[phase, g, LAST], r.at[4])
        landed(from_right.at[phase, g, FIRST], r.at[5])
        for i in range(2):
            landed(from_left.at[phase, g, A[i]], r.at[6 + i])
            landed(from_right.at[phase, g, B[i]], r.at[8 + i])
        summed[phase, g] = chunks[phase, g, 3] + from_left[phase, g] + from_right[phase, g]

    def sum_of(a):
        return ((a[0] + a[1]) + (a[2] + a[3])) + ((a[4] + a[5]) + (a[6] + a[7]))

    def stage_spread(g):
        sum_x(0, g)
        for o in z_order:
            j = along_z(o)
            send(summed.at[0, g, j], arrived.at[0, g, z], z_send.at[0, g], z_recv.at[0, g], (row, j * 4 + x))
        arrived[0, g, z] = summed[0, g, z]

    def stage_collect(g):
        landed(arrived.at[0, g, pl.ds(0, 7)], z_recv.at[0, g])
        mine = blocks.at[g, x, z]
        mine[...] = sum_of(arrived.at[0, g])
        for o in z_order[::-1]:
            j = along_z(o)
            send(mine, mine, zg_send.at[g], zg_recv.at[g, z], (row, j * 4 + x))
        forward(g, 0)

    def forward(g, *offsets):
        for o in offsets:
            j = along_z(o)
            piece = blocks.at[g, x, j]
            if o:
                landed(piece, zg_recv.at[g, j])
            send(piece, piece, xg_send.at[g], xg_recv.at[g, 0, j], right)
            send(piece, piece, xg_send.at[g], xg_recv.at[g, 1, j], left)

    def onward(g, *offsets):
        for o in offsets:
            j = along_z(o)
            back, at, way = (3, 0, right) if o < 4 else (1, 1, left)
            piece = blocks.at[g, along_x(back), j]
            landed(piece, xg_recv.at[g, at, j])
            send(piece, piece, xg_send.at[g], xg_recv.at[g, 2, j], way)

    def adjoint(g, ahead):
        block = along_x(ahead)
        high, low = factors(1, blocks[g, block])
        return times(high, low, density_high[block], density_low[block], 0)

    def stage_own(g):
        sums[g] = adjoint(g, 0)

    def stage_next(g):
        for o in range(8):
            j = along_z(o)
            back, at = (1, 1) if o < 4 else (3, 0)
            landed(blocks.at[g, along_x(back), j], xg_recv.at[g, at, j])
        sums[g] = sums[g] + (adjoint(g, 1) + adjoint(g, 3))

    def stage_far(g):
        for o in range(8):
            j = along_z(o)
            landed(blocks.at[g, along_x(2), j], xg_recv.at[g, 2, j])
        store(summed.at[1, g], sums[g] + adjoint(g, 2))
        for p in peers:
            send(summed.at[1, g, p], turned.at[1, g, row], y_send.at[1, g], y_recv.at[1, g, 0], (p, col))
        turned[1, g, row] = summed[1, g, row]

    def stage_join(g):
        landed(turned.at[1, g, pl.ds(0, 7)], y_recv.at[1, g, 0])
        gather(1, g, sum_of(turned.at[1, g]))

    def gather(phase, g, value):
        mine = gathered.at[phase, g, row]
        mine[...] = value
        for p in peers:
            send(mine, mine, g_send.at[phase, g], g_recv.at[phase, g], (p, col))

    def to_z(g, block, source):
        @pl.when(block != z)
        def _():
            pltpu.make_async_remote_copy(
                src_ref=source, dst_ref=arrived.at[2, g, z],
                send_sem=z_send.at[2, g], recv_sem=z_recv.at[2, g],
                device_id=(row, block * 4 + x), device_id_type=MESH,
            ).start()

    def stage_y(g):
        sum_x(2, g)
        for p in peers:
            send(summed.at[2, g, p], turned.at[2, g, row], y_send.at[2, g], y_recv.at[2, g, row], (p, col))
        turned[2, g, row] = summed[2, g, row]
        to_z(g, row, summed.at[2, g, row])

    def stage_z(g):
        for p in from_peers:
            piece = turned.at[2, g, p]
            landed(piece, y_recv.at[2, g, p])
            to_z(g, p, piece)
        arrived[2, g, z] = turned[2, g, z]

    def stage_gather(g):
        landed(arrived.at[2, g, pl.ds(0, 7)], z_recv.at[2, g])
        gather(2, g, sum_of(arrived.at[2, g]) + gathered[1, g, row])

    def stage_density(g):
        if g == 0:
            density_load.wait()

            def part(i, carry):
                for j in range(2):
                    h, l = split(density[j, rows_of(i), :])
                    density_high[i, j * COLS : (j + 1) * COLS] = h
                    density_low[i, j * COLS : (j + 1) * COLS] = l
                return carry

            lax.fori_loop(0, ROWS // COLS, part, 0)

    def stage_out(g):
        landed(gathered.at[2, g, pl.ds(0, 7)], g_recv.at[2, g])
        part, each = gathered[2, g], KINDS * 8
        for j in range(2):
            half = part[:, j * 8 : (j + 1) * 8]
            cuts = [half[i * KINDS : (i + 1) * KINDS].reshape(each, WIDE) for i in range(CUTS)]
            whole = jnp.concatenate(cuts, axis=1) if CUTS > 1 else cuts[0]
            out[j, :, g * each : (g + 1) * each] = whole.T

    def sent(g):
        seven = pl.ds(0, 7)
        for phase in (0, 2):
            landed(chunks.at[phase, g, pl.ds(0, 3)], x_send.at[phase, g])
            landed(arrived.at[phase, g, seven], z_send.at[phase, g])
        for phase in (1, 2):
            landed(turned.at[phase, g, seven], y_send.at[phase, g])
            landed(gathered.at[phase, g, seven], g_send.at[phase, g])
        landed(arrived.at[0, g, seven], zg_send.at[g])
        landed(blocks.at[g, pl.ds(0, 3)], xg_send.at[g])

    plan = (
        (0, functools.partial(stage_x, 0)),
        (3.7, functools.partial(stage_relay, 0)),
        (4.2, stage_density),
        (7.0, stage_spread),
        (12.1, stage_collect),
        (15.5, lambda g: forward(g, 1, 7)),
        (15.6, lambda g: onward(g, 0)),
        (16.3, lambda g: forward(g, 2, 6)),
        (17.1, lambda g: forward(g, 3, 5)),
        (18.0, lambda g: forward(g, 4)),
        (18.1, stage_own),
        (18.2, lambda g: onward(g, 1, 7)),
        (19.0, lambda g: onward(g, 2, 6)),
        (19.9, lambda g: onward(g, 3, 5)),
        (20.9, lambda g: onward(g, 4)),
        (21.1, stage_next),
        (24, stage_far),
        (29, stage_join),
        (34, functools.partial(stage_x, 2)),
        (38.3, functools.partial(stage_relay, 2)),
        (42, stage_y),
        (46.5, stage_z),
        (51.5, stage_gather),
        (56, stage_out),
    )
    turns = [(at + g * APART, g, stage) for at, stage in plan for g in range(GROUPS)]
    for _, g, stage in sorted(turns, key=lambda turn: turn[0]):
        stage(g)
    for g in range(GROUPS):
        sent(g)


def step(fock, density, probe):
    f32, bf16 = jnp.float32, jnp.bfloat16
    vmem, dma = pltpu.VMEM, pltpu.SemaphoreType.DMA
    each = (PHASES, GROUPS)
    piece = (DEPTH, WIDE)
    return pl.pallas_call(
        kernel,
        out_shape=jax.ShapeDtypeStruct(probe.shape, f32),
        in_specs=[pl.BlockSpec(memory_space=pltpu.HBM)] * 3,
        out_specs=pl.BlockSpec(memory_space=pltpu.VMEM),
        scratch_shapes=[
            vmem(fock.shape, f32), vmem(density.shape, f32), vmem(probe.shape, f32),
            vmem((ROWS, 2 * COLS), bf16), vmem((ROWS, 2 * COLS), bf16),
            vmem((ROWS // COLS, 2 * COLS, COLS), bf16), vmem((ROWS // COLS, 2 * COLS, COLS), bf16),
            vmem((GROUPS, PIECES, *piece), f32),
            vmem((*each, 4, PIECES, *piece), f32),
            vmem((*each, 2, 2, *piece), f32), vmem((*each, 2, 2, *piece), f32),
            vmem((*each, PIECES, *piece), f32), vmem((*each, PIECES, *piece), f32),
            vmem((*each, PIECES, *piece), f32), vmem((*each, PIECES, *piece), f32),
            vmem((*each, 8, *piece), f32), vmem((GROUPS, 4, PIECES, *piece), f32),
            vmem((GROUPS, TALL, COLS), f32), vmem((*each, PIECES, *piece), f32),
            dma((6,)), dma(each), dma((*each, 10)), dma(each), dma((*each, PIECES)),
            dma(each), dma(each), dma(each), dma(each),
            dma((GROUPS,)), dma((GROUPS, 8)), dma((GROUPS,)), dma((GROUPS, 3, 8)),
        ],
        compiler_params=pltpu.CompilerParams(
            collective_id=0, has_side_effects=True, vmem_limit_bytes=VMEM_LIMIT
        ),
    )(fock, density, probe)


def solution(mesh):
    return jax.shard_map(
        step,
        mesh=mesh,
        in_specs=(P(None, "row", "col"), P(None, "row", "col"), P(None, "col", None)),
        out_specs=P(None, "col", None),
        check_vma=False,
    )
```

```python
import functools

import jax
import jax.numpy as jnp
from jax import lax
from jax.experimental import pallas as pl
from jax.experimental.pallas import tpu as pltpu
from jax.sharding import PartitionSpec as P

MESH = pl.DeviceIdType.MESH
DT = 0.5
ROWS = 1024
COLS = 256
PIECES = 8
DEPTH = 16
GROUPS = 4
CUTS = GROUPS // 2
WIDE = COLS // CUTS
KINDS = PIECES // CUTS
TALL = KINDS * DEPTH
PHASES = 3
WAVES = (0, 1, 2, 3, 4, 3, 2, 1)
LATER, FAR = 5, 6
VMEM_LIMIT = 60 * 1024 * 1024
ORDER = (
    0, 4, 1, 8, 12, 2, 9, 13, 3, 16, 20, 10, 14, 21, 11, 15,
    22, 24, 23, 25, 44, 28, 26, 32, 45, 36, 29, 48, 40, 64, 27, 33,
    46, 52, 30, 37, 56, 34, 49, 60, 68, 41, 65, 38, 31, 47, 53, 42,
    50, 66, 35, 57, 54, 72, 61, 69, 58, 39, 51, 43, 67, 62, 70, 55,
    73, 59, 76, 63, 71, 74, 75, 77, 80, 78, 79, 84, 88, 81, 82, 92,
    83, 85, 89, 86, 90, 87, 96, 91, 93, 94, 95, 97, 98, 100, 99, 104,
    101, 102, 103, 105, 106, 107,
)


def split(value):
    high = value.astype(jnp.bfloat16)
    return high, (value - high.astype(jnp.float32)).astype(jnp.bfloat16)


def flat(vector):
    parts = [vector[i * KINDS : (i + 1) * KINDS].reshape(TALL, WIDE) for i in range(CUTS)]
    return jnp.concatenate(parts, axis=1) if CUTS > 1 else parts[0]


def factors(phase, vector):
    real, imag = vector[:, :8], vector[:, 8:]
    if phase == 1:
        first, second = (real, imag), (imag, -real)
    else:
        dt = DT if phase == 0 else -DT
        first, second = (-dt * imag, dt * real), (-dt * real, -dt * imag)
    first = flat(jnp.concatenate(first, axis=1))
    second = flat(jnp.concatenate(second, axis=1))
    return split(jnp.concatenate([first, second], axis=1))


def times(high, low, matrix_high, matrix_low, depth_dim):
    dot = functools.partial(
        lax.dot_general,
        dimension_numbers=(((1,), (depth_dim,)), ((), ())),
        preferred_element_type=jnp.float32,
    )
    both = dot(jnp.concatenate([high, low], axis=0), matrix_high)
    return both[:TALL] + (both[TALL:] + dot(high, matrix_low))


def kernel(
    fock_hbm, density_hbm, probe_hbm, out,
    fock, density, probe, fock_high, fock_low, turned_high, turned_low, density_high, density_low,
    start, chunks, relay_a, relay_b, from_left, from_right, summed, turned, arrived, blocks, sums, gathered,
    load_sem, x_send, x_recv, y_send, y_one, y_recv, z_send, z_recv, g_send, g_recv, zg_send, zg_recv, xg_send, xg_recv,
):
    row, col = lax.axis_index("row"), lax.axis_index("col")
    z, x = col // 4, lax.rem(col, 4)
    y, core = row // 2, lax.rem(row, 2)
    right = (row, z * 4 + lax.rem(x + 1, 4))
    left = (row, z * 4 + lax.rem(x + 3, 4))

    def along_x(ahead):
        return lax.rem(x + ahead, 4)

    def along_z(ahead):
        return lax.rem(z + ahead, 8)

    def peer(dy, dc):
        return lax.rem(y + dy, 4) * 2 + lax.rem(core + dc, 2)

    peers = [peer(*d) for d in ((2, 0), (2, 1), (1, 0), (3, 0), (1, 1), (3, 1), (0, 1))]
    from_peers = [peer(*d) for d in ((0, 1), (1, 0), (3, 0), (1, 1), (3, 1), (2, 0), (2, 1))]
    z_order = (4, 3, 5, 2, 6, 1, 7)

    barrier = pltpu.get_barrier_semaphore()

    def hello(r, c):
        pl.semaphore_signal(barrier, inc=1, device_id=(r, c), device_id_type=MESH)

    for j in z_order:
        hello(row, along_z(j) * 4 + x)
    for p in peers:
        hello(p, col)
    hello(*right)
    hello(*left)

    def rows_of(block):
        return pl.ds(pl.multiple_of(block * COLS, COLS), COLS)

    probe_load = pltpu.make_async_copy(probe_hbm, probe, load_sem.at[0])
    density_load = pltpu.make_async_copy(density_hbm, density, load_sem.at[1])
    fock_loads = {}
    probe_load.start()
    for i, ahead in enumerate((2, 1, 3, 0)):
        rows = rows_of(along_x(ahead))
        fock_loads[ahead] = pltpu.make_async_copy(fock_hbm.at[:, rows, :], fock.at[:, rows, :], load_sem.at[2 + i])
        fock_loads[ahead].start()

    probe_load.wait()
    for j in range(2):
        probe_t = probe[j].T.reshape(GROUPS, KINDS, 8, COLS)
        for i in range(CUTS):
            start[:, i * KINDS : (i + 1) * KINDS, j * 8 : (j + 1) * 8, :] = probe_t[..., i * WIDE : (i + 1) * WIDE]

    def send(source, target, send_sem, recv_sem, device):
        copy = pltpu.make_async_remote_copy(
            src_ref=source, dst_ref=target, send_sem=send_sem, recv_sem=recv_sem,
            device_id=device, device_id_type=MESH,
        )
        copy.start()

    def landed(target, sem):
        pltpu.make_async_copy(target, target, sem).wait()

    def store(box, value):
        for i in range(CUTS):
            box[i * KINDS : (i + 1) * KINDS] = value[:, i * WIDE : (i + 1) * WIDE].reshape(KINDS, DEPTH, WIDE)

    FIRST, LAST = pl.ds(0, 4), pl.ds(4, 4)
    A, B = (pl.ds(0, 2), pl.ds(2, 2)), (pl.ds(4, 2), pl.ds(6, 2))

    def stage_x(phase, g):
        if phase == 0:
            vector = start[g]
        else:
            landed(gathered.at[1, g, pl.ds(0, 7)], g_recv.at[0, g])
            vector = gathered[1, g]
        high, low = factors(phase, vector)
        box = chunks.at[phase, g]
        s, r = x_send.at[phase // 2], x_recv.at[phase // 2, g]

        def one(slot, ahead):
            rows = rows_of(along_x(ahead))
            if phase == 0 and g == 0:
                fock_loads[ahead].wait()
                for j in range(2):
                    h, l = split(fock[j, rows, :])
                    fock_high[rows, j * COLS : (j + 1) * COLS] = h
                    fock_low[rows, j * COLS : (j + 1) * COLS] = l
                value = times(high, low, fock_high[rows, :], fock_low[rows, :], 1)
            else:
                block = along_x(ahead)
                value = times(high, low, turned_high[block], turned_low[block], 0)
            store(box.at[slot], value)

        one(0, 2)
        if phase == 0 and g == 0:
            pl.semaphore_wait(barrier, 16)
        for i in range(2):
            send(box.at[0, A[i]], relay_a.at[phase, g, i], s, r.at[i], right)
            send(box.at[0, B[i]], relay_b.at[phase, g, i], s, r.at[2 + i], left)
        one(1, 1)
        send(box.at[1, LAST], from_left.at[phase, g, LAST], s, r.at[4], right)
        one(2, 3)
        send(box.at[2, FIRST], from_right.at[phase, g, FIRST], s, r.at[5], left)
        one(3, 0)
        if phase == 0:
            if g == 0:
                density_load.start()

            @pl.when(z == row)
            def _():
                box[3] = box[3] + start[g]

    def stage_relay(phase, i, g):
        box = chunks.at[phase, g]
        s, r = x_send.at[phase // 2], x_recv.at[phase // 2, g]
        landed(relay_a.at[phase, g, i], r.at[i])
        box[1, A[i]] = box[1, A[i]] + relay_a[phase, g, i]
        send(box.at[1, A[i]], from_left.at[phase, g, A[i]], s, r.at[4], right)
        landed(relay_b.at[phase, g, i], r.at[2 + i])
        box[2, B[i]] = box[2, B[i]] + relay_b[phase, g, i]
        send(box.at[2, B[i]], from_right.at[phase, g, B[i]], s, r.at[5], left)

    def sum_x(phase, g):
        r = x_recv.at[phase // 2, g]
        landed(from_left.at[phase, g], r.at[4])
        landed(from_right.at[phase, g], r.at[5])
        summed[phase, g] = chunks[phase, g, 3] + from_left[phase, g] + from_right[phase, g]

    def sum_of(a):
        return ((a[0] + a[1]) + (a[2] + a[3])) + ((a[4] + a[5]) + (a[6] + a[7]))

    def stage_spread(g):
        sum_x(0, g)
        for o in z_order:
            j = along_z(o)
            send(summed.at[0, g, j], arrived.at[0, g, z], z_send.at[0], z_recv.at[0, g], (row, j * 4 + x))
        arrived[0, g, z] = summed[0, g, z]

    def stage_collect(g):
        landed(arrived.at[0, g, pl.ds(0, 7)], z_recv.at[0, g])
        mine = blocks.at[g, x, z]
        mine[...] = sum_of(arrived.at[0, g])
        for o in z_order[::-1]:
            j = along_z(o)
            send(mine, mine, zg_send, zg_recv.at[g, min(o, 8 - o) - 1], (row, j * 4 + x))
        forward(g, 0)

    def forward(g, *offsets):
        if offsets[0]:
            landed(arrived.at[0, g, pl.ds(0, len(offsets))], zg_recv.at[g, offsets[0] - 1])
        for o in offsets:
            j = along_z(o)
            piece = blocks.at[g, x, j]
            first, second = (WAVES[o], LATER) if o < 4 else (LATER, WAVES[o])
            send(piece, piece, xg_send, xg_recv.at[g, first], right)
            send(piece, piece, xg_send, xg_recv.at[g, second], left)

    def onward(g, *offsets):
        landed(arrived.at[0, g, pl.ds(0, len(offsets))], xg_recv.at[g, offsets[0]])
        for o in offsets:
            back, way = (3, right) if o < 4 else (1, left)
            piece = blocks.at[g, along_x(back), along_z(o)]
            send(piece, piece, xg_send, xg_recv.at[g, FAR], way)

    def adjoint(g, ahead):
        block = along_x(ahead)
        high, low = factors(1, blocks[g, block])
        return times(high, low, density_high[block], density_low[block], 0)

    def stage_own(g):
        sums[g] = adjoint(g, 0)

    def stage_next(g):
        landed(blocks.at[g, 0], xg_recv.at[g, LATER])
        sums[g] = sums[g] + (adjoint(g, 1) + adjoint(g, 3))

    def stage_far(g):
        landed(blocks.at[g, 0], xg_recv.at[g, FAR])
        store(summed.at[1, g], sums[g] + adjoint(g, 2))
        for p in peers:
            send(summed.at[1, g, p], turned.at[1, g, row], y_send.at[0], y_one.at[g], (p, col))
        turned[1, g, row] = summed[1, g, row]

    def stage_join(g):
        landed(turned.at[1, g, pl.ds(0, 7)], y_one.at[g])
        gather(1, g, sum_of(turned.at[1, g]))

    def gather(phase, g, value):
        mine = gathered.at[phase, g, row]
        mine[...] = value
        for p in peers:
            send(mine, mine, g_send.at[phase - 1], g_recv.at[phase - 1, g], (p, col))

    def to_z(g, block, source):
        @pl.when(block != z)
        def _():
            pltpu.make_async_remote_copy(
                src_ref=source, dst_ref=arrived.at[2, g, z],
                send_sem=z_send.at[1], recv_sem=z_recv.at[1, g],
                device_id=(row, block * 4 + x), device_id_type=MESH,
            ).start()

    def stage_y(g):
        sum_x(2, g)
        for p in peers:
            send(summed.at[2, g, p], turned.at[2, g, row], y_send.at[1], y_recv.at[g, row], (p, col))
        turned[2, g, row] = summed[2, g, row]
        to_z(g, row, summed.at[2, g, row])

    def stage_z(g):
        for p in from_peers:
            piece = turned.at[2, g, p]
            landed(piece, y_recv.at[g, p])
            to_z(g, p, piece)
        arrived[2, g, z] = turned[2, g, z]

    def stage_gather(g):
        landed(arrived.at[2, g, pl.ds(0, 7)], z_recv.at[1, g])
        gather(2, g, sum_of(arrived.at[2, g]) + gathered[1, g, row])

    def stage_turn(g):
        for i in range(ROWS // COLS):
            for j in range(2):
                h, l = split(fock[j, i * COLS : (i + 1) * COLS, :].T)
                turned_high[i, j * COLS : (j + 1) * COLS] = h
                turned_low[i, j * COLS : (j + 1) * COLS] = l

    def stage_density(g):
        if g == 0:
            density_load.wait()

            def part(i, carry):
                for j in range(2):
                    h, l = split(density[j, rows_of(i), :])
                    density_high[i, j * COLS : (j + 1) * COLS] = h
                    density_low[i, j * COLS : (j + 1) * COLS] = l
                return carry

            lax.fori_loop(0, ROWS // COLS, part, 0)

    def stage_out(g):
        landed(gathered.at[2, g, pl.ds(0, 7)], g_recv.at[1, g])
        part, each = gathered[2, g], KINDS * 8
        for j in range(2):
            half = part[:, j * 8 : (j + 1) * 8]
            cuts = [half[i * KINDS : (i + 1) * KINDS].reshape(each, WIDE) for i in range(CUTS)]
            whole = jnp.concatenate(cuts, axis=1) if CUTS > 1 else cuts[0]
            out[j, :, g * each : (g + 1) * each] = whole.T

    def sent():
        every, seven = pl.ds(0, GROUPS), pl.ds(0, 7)
        for i in range(2):
            landed(chunks.at[0, every, pl.ds(0, 3)], x_send.at[i])
            for sem in (y_send, z_send, g_send):
                landed(arrived.at[0, every, seven], sem.at[i])
        landed(arrived.at[0, every, seven], zg_send)
        landed(blocks.at[every, pl.ds(0, 3)], xg_send)

    plan = (
        functools.partial(stage_x, 0),
        stage_turn,
        functools.partial(stage_relay, 0, 0),
        functools.partial(stage_relay, 0, 1),
        stage_density,
        stage_spread,
        stage_collect,
        lambda g: forward(g, 1, 7),
        lambda g: forward(g, 2, 6),
        lambda g: forward(g, 3, 5),
        lambda g: forward(g, 4),
        lambda g: onward(g, 0),
        lambda g: onward(g, 1, 7),
        lambda g: onward(g, 2, 6),
        lambda g: onward(g, 3, 5),
        lambda g: onward(g, 4),
        stage_own,
        stage_next,
        stage_far,
        stage_join,
        functools.partial(stage_x, 2),
        functools.partial(stage_relay, 2, 0),
        functools.partial(stage_relay, 2, 1),
        stage_y,
        stage_z,
        stage_gather,
        stage_out,
    )
    for turn in ORDER:
        plan[turn // 4](turn % 4)
    sent()


def step(fock, density, probe):
    f32, bf16 = jnp.float32, jnp.bfloat16
    vmem, dma = pltpu.VMEM, pltpu.SemaphoreType.DMA
    each = (PHASES, GROUPS)
    piece = (DEPTH, WIDE)
    return pl.pallas_call(
        kernel,
        out_shape=jax.ShapeDtypeStruct(probe.shape, f32),
        in_specs=[pl.BlockSpec(memory_space=pltpu.HBM)] * 3,
        out_specs=pl.BlockSpec(memory_space=pltpu.VMEM),
        scratch_shapes=[
            vmem(fock.shape, f32), vmem(density.shape, f32), vmem(probe.shape, f32),
            vmem((ROWS, 2 * COLS), bf16), vmem((ROWS, 2 * COLS), bf16),
            vmem((ROWS // COLS, 2 * COLS, COLS), bf16), vmem((ROWS // COLS, 2 * COLS, COLS), bf16),
            vmem((ROWS // COLS, 2 * COLS, COLS), bf16), vmem((ROWS // COLS, 2 * COLS, COLS), bf16),
            vmem((GROUPS, PIECES, *piece), f32),
            vmem((*each, 4, PIECES, *piece), f32),
            vmem((*each, 2, 2, *piece), f32), vmem((*each, 2, 2, *piece), f32),
            vmem((*each, PIECES, *piece), f32), vmem((*each, PIECES, *piece), f32),
            vmem((*each, PIECES, *piece), f32), vmem((*each, PIECES, *piece), f32),
            vmem((*each, 8, *piece), f32), vmem((GROUPS, 4, PIECES, *piece), f32),
            vmem((GROUPS, TALL, COLS), f32), vmem((*each, PIECES, *piece), f32),
            dma((6,)), dma((2,)), dma((2, GROUPS, 6)), dma((2,)), dma((GROUPS,)), dma((GROUPS, PIECES)),
            dma((2,)), dma((2, GROUPS)), dma((2,)), dma((2, GROUPS)),
            dma, dma((GROUPS, 4)), dma, dma((GROUPS, 7)),
        ],
        compiler_params=pltpu.CompilerParams(
            collective_id=0, has_side_effects=True, vmem_limit_bytes=VMEM_LIMIT
        ),
    )(fock, density, probe)


def solution(mesh):
    return jax.shard_map(
        step,
        mesh=mesh,
        in_specs=(P(None, "row", "col"), P(None, "row", "col"), P(None, "col", None)),
        out_specs=P(None, "col", None),
        check_vma=False,
    )
```

```python
import functools

import jax
import jax.numpy as jnp
from jax import lax
from jax.experimental import pallas as pl
from jax.experimental.pallas import tpu as pltpu
from jax.sharding import PartitionSpec as P

MESH = pl.DeviceIdType.MESH
DT = 0.5
ROWS = 1024
COLS = 256
PIECES = 8
DEPTH = 16
GROUPS = 4
CUTS = GROUPS // 2
WIDE = COLS // CUTS
KINDS = PIECES // CUTS
TALL = KINDS * DEPTH
PHASES = 3
VMEM_LIMIT = 60 * 1024 * 1024
ORDER = (
    0, 4, 1, 2, 3, 8, 12, 13, 16, 14, 17, 20, 15, 24, 28, 21,
    32, 36, 18, 25, 29, 33, 37, 19, 22, 40, 44, 26, 30, 41, 23, 45,
    34, 38, 27, 48, 31, 35, 39, 42, 49, 46, 52, 43, 47, 53, 50, 51,
    56, 54, 57, 55, 60, 61, 58, 59, 64, 62, 65, 63, 68, 69, 66, 67,
    70, 71,
)


def split(value):
    high = value.astype(jnp.bfloat16)
    return high, (value - high.astype(jnp.float32)).astype(jnp.bfloat16)


def flat(vector):
    parts = [vector[i * KINDS : (i + 1) * KINDS].reshape(TALL, WIDE) for i in range(CUTS)]
    return jnp.concatenate(parts, axis=1) if CUTS > 1 else parts[0]


def factors(phase, vector):
    real, imag = vector[:, :8], vector[:, 8:]
    if phase == 1:
        first, second = (real, imag), (imag, -real)
    else:
        dt = DT if phase == 0 else -DT
        first, second = (-dt * imag, dt * real), (-dt * real, -dt * imag)
    first = flat(jnp.concatenate(first, axis=1))
    second = flat(jnp.concatenate(second, axis=1))
    return split(jnp.concatenate([first, second], axis=1))


def times(high, low, matrix_high, matrix_low, depth_dim):
    dot = functools.partial(
        lax.dot_general,
        dimension_numbers=(((1,), (depth_dim,)), ((), ())),
        preferred_element_type=jnp.float32,
    )
    both = dot(jnp.concatenate([high, low], axis=0), matrix_high)
    return both[:TALL] + (both[TALL:] + dot(high, matrix_low))


def kernel(
    fock_hbm, density_hbm, probe_hbm, out,
    fock, density, probe, fock_high, fock_low, turned_high, turned_low, density_high, density_low,
    start, chunks, from_far, from_left, from_right, summed, turned, arrived, blocks, sums, gathered,
    load_sem, x_send, x_recv, y_send, y_one, y_recv, z_send, z_recv, g_send, g_recv, zg_send, zg_recv, xg_send, xg_recv,
):
    row, col = lax.axis_index("row"), lax.axis_index("col")
    z, x = col // 4, lax.rem(col, 4)
    y, core = row // 2, lax.rem(row, 2)
    right = (row, z * 4 + lax.rem(x + 1, 4))
    left = (row, z * 4 + lax.rem(x + 3, 4))
    far = (row, z * 4 + lax.rem(x + 2, 4))

    def along_x(ahead):
        return lax.rem(x + ahead, 4)

    def along_z(ahead):
        return lax.rem(z + ahead, 8)

    def peer(dy, dc):
        return lax.rem(y + dy, 4) * 2 + lax.rem(core + dc, 2)

    peers = [peer(*d) for d in ((2, 0), (2, 1), (1, 0), (3, 0), (1, 1), (3, 1), (0, 1))]
    from_peers = [peer(*d) for d in ((0, 1), (1, 0), (3, 0), (1, 1), (3, 1), (2, 0), (2, 1))]
    z_order = (4, 3, 5, 2, 6, 1, 7)

    barrier = pltpu.get_barrier_semaphore()

    def hello(r, c):
        pl.semaphore_signal(barrier, inc=1, device_id=(r, c), device_id_type=MESH)

    for j in z_order:
        hello(row, along_z(j) * 4 + x)
    for p in peers:
        hello(p, col)
    hello(*far)
    hello(*right)
    hello(*left)

    def rows_of(block):
        return pl.ds(pl.multiple_of(block * COLS, COLS), COLS)

    probe_load = pltpu.make_async_copy(probe_hbm, probe, load_sem.at[0])
    density_load = pltpu.make_async_copy(density_hbm, density, load_sem.at[1])
    fock_loads = {}
    probe_load.start()
    for i, ahead in enumerate((2, 1, 3, 0)):
        rows = rows_of(along_x(ahead))
        fock_loads[ahead] = pltpu.make_async_copy(fock_hbm.at[:, rows, :], fock.at[:, rows, :], load_sem.at[2 + i])
        fock_loads[ahead].start()

    probe_load.wait()
    for j in range(2):
        probe_t = probe[j].T.reshape(GROUPS, KINDS, 8, COLS)
        for i in range(CUTS):
            start[:, i * KINDS : (i + 1) * KINDS, j * 8 : (j + 1) * 8, :] = probe_t[..., i * WIDE : (i + 1) * WIDE]

    def send(source, target, send_sem, recv_sem, device):
        copy = pltpu.make_async_remote_copy(
            src_ref=source, dst_ref=target, send_sem=send_sem, recv_sem=recv_sem,
            device_id=device, device_id_type=MESH,
        )
        copy.start()

    def landed(target, sem):
        pltpu.make_async_copy(target, target, sem).wait()

    def store(box, value):
        for i in range(CUTS):
            box[i * KINDS : (i + 1) * KINDS] = value[:, i * WIDE : (i + 1) * WIDE].reshape(KINDS, DEPTH, WIDE)

    def stage_x(phase, g):
        if phase == 0:
            vector = start[g]
        else:
            landed(gathered.at[1, g, pl.ds(0, 7)], g_recv.at[0, g])
            vector = gathered[1, g]
        high, low = factors(phase, vector)
        box = chunks.at[phase, g]
        s, r = x_send.at[phase // 2], x_recv.at[phase // 2, g]

        def one(slot, ahead):
            rows = rows_of(along_x(ahead))
            if phase == 0 and g == 0:
                fock_loads[ahead].wait()
                for j in range(2):
                    h, l = split(fock[j, rows, :])
                    fock_high[rows, j * COLS : (j + 1) * COLS] = h
                    fock_low[rows, j * COLS : (j + 1) * COLS] = l
                value = times(high, low, fock_high[rows, :], fock_low[rows, :], 1)
            else:
                block = along_x(ahead)
                value = times(high, low, turned_high[block], turned_low[block], 0)
            store(box.at[slot], value)

        one(0, 2)
        if phase == 0 and g == 0:
            pl.semaphore_wait(barrier, 17)
        send(box.at[0], from_far.at[phase, g], s, r, far)
        one(1, 1)
        send(box.at[1], from_left.at[phase, g], s, r, right)
        one(2, 3)
        send(box.at[2], from_right.at[phase, g], s, r, left)
        one(3, 0)
        if phase == 0:
            if g == 0:
                density_load.start()

            @pl.when(z == row)
            def _():
                box[3] = box[3] + start[g]

    def sum_x(phase, g):
        landed(chunks.at[phase, g, pl.ds(0, 3)], x_recv.at[phase // 2, g])
        near = from_left[phase, g] + from_right[phase, g]
        summed[phase, g] = (chunks[phase, g, 3] + from_far[phase, g]) + near

    def sum_of(a):
        return ((a[0] + a[1]) + (a[2] + a[3])) + ((a[4] + a[5]) + (a[6] + a[7]))

    def stage_spread(g):
        sum_x(0, g)
        for o in z_order:
            j = along_z(o)
            send(summed.at[0, g, j], arrived.at[0, g, z], z_send.at[0], z_recv.at[0, g], (row, j * 4 + x))
        arrived[0, g, z] = summed[0, g, z]

    def stage_collect(g):
        landed(arrived.at[0, g, pl.ds(0, 7)], z_recv.at[0, g])
        mine = blocks.at[g, x, z]
        mine[...] = sum_of(arrived.at[0, g])
        for o in z_order[::-1]:
            j = along_z(o)
            send(mine, mine, zg_send, zg_recv.at[g, min(o, 8 - o) - 1], (row, j * 4 + x))
        forward(g, 0)

    def forward(g, *offsets):
        if offsets[0]:
            landed(arrived.at[0, g, pl.ds(0, len(offsets))], zg_recv.at[g, offsets[0] - 1])
        for o in offsets:
            j = along_z(o)
            piece = blocks.at[g, x, j]
            send(piece, piece, xg_send, xg_recv.at[g, 1], far)
            send(piece, piece, xg_send, xg_recv.at[g, 0], right)
            send(piece, piece, xg_send, xg_recv.at[g, 0], left)

    def adjoint(g, ahead):
        block = along_x(ahead)
        high, low = factors(1, blocks[g, block])
        return times(high, low, density_high[block], density_low[block], 0)

    def stage_own(g):
        sums[g] = adjoint(g, 0)

    def stage_next(g):
        landed(blocks.at[g, pl.ds(0, 2)], xg_recv.at[g, 0])
        sums[g] = sums[g] + (adjoint(g, 1) + adjoint(g, 3))

    def stage_far(g):
        landed(blocks.at[g, 0], xg_recv.at[g, 1])
        store(summed.at[1, g], sums[g] + adjoint(g, 2))
        for p in peers:
            send(summed.at[1, g, p], turned.at[1, g, row], y_send.at[0], y_one.at[g], (p, col))
        turned[1, g, row] = summed[1, g, row]

    def stage_join(g):
        landed(turned.at[1, g, pl.ds(0, 7)], y_one.at[g])
        gather(1, g, sum_of(turned.at[1, g]))

    def gather(phase, g, value):
        mine = gathered.at[phase, g, row]
        mine[...] = value
        for p in peers:
            send(mine, mine, g_send.at[phase - 1], g_recv.at[phase - 1, g], (p, col))

    def to_z(g, block, source):
        @pl.when(block != z)
        def _():
            pltpu.make_async_remote_copy(
                src_ref=source, dst_ref=arrived.at[2, g, z],
                send_sem=z_send.at[1], recv_sem=z_recv.at[1, g],
                device_id=(row, block * 4 + x), device_id_type=MESH,
            ).start()

    def stage_y(g):
        sum_x(2, g)
        for p in peers:
            send(summed.at[2, g, p], turned.at[2, g, row], y_send.at[1], y_recv.at[g, row], (p, col))
        turned[2, g, row] = summed[2, g, row]
        to_z(g, row, summed.at[2, g, row])

    def stage_z(g):
        for p in from_peers:
            piece = turned.at[2, g, p]
            landed(piece, y_recv.at[g, p])
            to_z(g, p, piece)
        arrived[2, g, z] = turned[2, g, z]

    def stage_gather(g):
        landed(arrived.at[2, g, pl.ds(0, 7)], z_recv.at[1, g])
        gather(2, g, sum_of(arrived.at[2, g]) + gathered[1, g, row])

    def stage_turn(g):
        for i in range(ROWS // COLS):
            for j in range(2):
                h, l = split(fock[j, i * COLS : (i + 1) * COLS, :].T)
                turned_high[i, j * COLS : (j + 1) * COLS] = h
                turned_low[i, j * COLS : (j + 1) * COLS] = l

    def stage_density(g):
        if g == 0:
            density_load.wait()

            def part(i, carry):
                for j in range(2):
                    h, l = split(density[j, rows_of(i), :])
                    density_high[i, j * COLS : (j + 1) * COLS] = h
                    density_low[i, j * COLS : (j + 1) * COLS] = l
                return carry

            lax.fori_loop(0, ROWS // COLS, part, 0)

    def stage_out(g):
        landed(gathered.at[2, g, pl.ds(0, 7)], g_recv.at[1, g])
        part, each = gathered[2, g], KINDS * 8
        for j in range(2):
            half = part[:, j * 8 : (j + 1) * 8]
            cuts = [half[i * KINDS : (i + 1) * KINDS].reshape(each, WIDE) for i in range(CUTS)]
            whole = jnp.concatenate(cuts, axis=1) if CUTS > 1 else cuts[0]
            out[j, :, g * each : (g + 1) * each] = whole.T

    def sent():
        every, seven = pl.ds(0, GROUPS), pl.ds(0, 7)
        for i in range(2):
            landed(chunks.at[0, every, pl.ds(0, 3)], x_send.at[i])
            for sem in (y_send, z_send, g_send):
                landed(arrived.at[0, every, seven], sem.at[i])
        landed(arrived.at[0, every, seven], zg_send)
        landed(blocks.at[every, pl.ds(0, 3)], xg_send)

    plan = (
        functools.partial(stage_x, 0),
        stage_turn,
        stage_density,
        stage_spread,
        stage_collect,
        lambda g: forward(g, 1, 7),
        lambda g: forward(g, 2, 6),
        lambda g: forward(g, 3, 5),
        lambda g: forward(g, 4),
        stage_own,
        stage_next,
        stage_far,
        stage_join,
        functools.partial(stage_x, 2),
        stage_y,
        stage_z,
        stage_gather,
        stage_out,
    )
    for turn in ORDER:
        plan[turn // 4](turn % 4)
    sent()


def step(fock, density, probe):
    f32, bf16 = jnp.float32, jnp.bfloat16
    vmem, dma = pltpu.VMEM, pltpu.SemaphoreType.DMA
    each = (PHASES, GROUPS)
    piece = (DEPTH, WIDE)
    return pl.pallas_call(
        kernel,
        out_shape=jax.ShapeDtypeStruct(probe.shape, f32),
        in_specs=[pl.BlockSpec(memory_space=pltpu.HBM)] * 3,
        out_specs=pl.BlockSpec(memory_space=pltpu.VMEM),
        scratch_shapes=[
            vmem(fock.shape, f32), vmem(density.shape, f32), vmem(probe.shape, f32),
            vmem((ROWS, 2 * COLS), bf16), vmem((ROWS, 2 * COLS), bf16),
            vmem((ROWS // COLS, 2 * COLS, COLS), bf16), vmem((ROWS // COLS, 2 * COLS, COLS), bf16),
            vmem((ROWS // COLS, 2 * COLS, COLS), bf16), vmem((ROWS // COLS, 2 * COLS, COLS), bf16),
            vmem((GROUPS, PIECES, *piece), f32),
            vmem((*each, 4, PIECES, *piece), f32),
            vmem((*each, PIECES, *piece), f32),
            vmem((*each, PIECES, *piece), f32), vmem((*each, PIECES, *piece), f32),
            vmem((*each, PIECES, *piece), f32), vmem((*each, PIECES, *piece), f32),
            vmem((*each, 8, *piece), f32), vmem((GROUPS, 4, PIECES, *piece), f32),
            vmem((GROUPS, TALL, COLS), f32), vmem((*each, PIECES, *piece), f32),
            dma((6,)), dma((2,)), dma((2, GROUPS)), dma((2,)), dma((GROUPS,)), dma((GROUPS, PIECES)),
            dma((2,)), dma((2, GROUPS)), dma((2,)), dma((2, GROUPS)),
            dma, dma((GROUPS, 4)), dma, dma((GROUPS, 2)),
        ],
        compiler_params=pltpu.CompilerParams(
            collective_id=0, has_side_effects=True, vmem_limit_bytes=VMEM_LIMIT
        ),
    )(fock, density, probe)


def solution(mesh):
    return jax.shard_map(
        step,
        mesh=mesh,
        in_specs=(P(None, "row", "col"), P(None, "row", "col"), P(None, "col", None)),
        out_specs=P(None, "col", None),
        check_vma=False,
    )
```

```python
import functools

import jax
import jax.numpy as jnp
from jax import lax
from jax.experimental import pallas as pl
from jax.experimental.pallas import tpu as pltpu
from jax.sharding import PartitionSpec as P

MESH = pl.DeviceIdType.MESH
DT = 0.5
ROWS = 1024
COLS = 256
PIECES = 8
DEPTH = 16
GROUPS = 4
CUTS = GROUPS // 2
WIDE = COLS // CUTS
KINDS = PIECES // CUTS
TALL = KINDS * DEPTH
PHASES = 3
VMEM_LIMIT = 60 * 1024 * 1024
ORDER = (
    0, 4, 1, 8, 12, 2, 3, 13, 16, 14, 17, 15, 20, 24, 28, 32,
    21, 36, 18, 25, 29, 33, 19, 40, 22, 44, 26, 37, 30, 34, 23, 41,
    45, 27, 48, 38, 31, 35, 39, 42, 46, 49, 52, 43, 47, 50, 53, 51,
    54, 55, 56, 57, 58, 60, 61, 59, 62, 63, 64, 66, 68, 65, 67, 70,
    69, 71,
)


def split(value):
    high = value.astype(jnp.bfloat16)
    return high, (value - high.astype(jnp.float32)).astype(jnp.bfloat16)


def flat(vector):
    parts = [vector[i * KINDS : (i + 1) * KINDS].reshape(TALL, WIDE) for i in range(CUTS)]
    return jnp.concatenate(parts, axis=1) if CUTS > 1 else parts[0]


def factors(phase, vector):
    real, imag = vector[:, :8], vector[:, 8:]
    if phase == 1:
        first, second = (real, imag), (imag, -real)
    else:
        dt = DT if phase == 0 else -DT
        first, second = (-dt * imag, dt * real), (-dt * real, -dt * imag)
    first = flat(jnp.concatenate(first, axis=1))
    second = flat(jnp.concatenate(second, axis=1))
    return split(jnp.concatenate([first, second], axis=1))


def times(high, low, matrix_high, matrix_low, depth_dim):
    dot = functools.partial(
        lax.dot_general,
        dimension_numbers=(((1,), (depth_dim,)), ((), ())),
        preferred_element_type=jnp.float32,
    )
    both = dot(jnp.concatenate([high, low], axis=0), matrix_high)
    return both[:TALL] + (both[TALL:] + dot(high, matrix_low))


def kernel(
    fock_hbm, density_hbm, probe_hbm, out,
    fock, density, probe, fock_high, fock_low, turned_high, turned_low, density_high, density_low,
    start, chunks, from_far, from_left, from_right, summed, turned, arrived, blocks, sums, gathered,
    load_sem, x_send, x_recv, y_send, y_one, y_recv, z_send, z_recv, g_send, g_recv, zg_send, zg_recv, xg_send, xg_recv,
):
    row, col = lax.axis_index("row"), lax.axis_index("col")
    z, x = col // 4, lax.rem(col, 4)
    y, core = row // 2, lax.rem(row, 2)
    right = (row, z * 4 + lax.rem(x + 1, 4))
    left = (row, z * 4 + lax.rem(x + 3, 4))
    far = (row, z * 4 + lax.rem(x + 2, 4))

    def along_x(ahead):
        return lax.rem(x + ahead, 4)

    def along_z(ahead):
        return lax.rem(z + ahead, 8)

    def peer(dy, dc):
        return lax.rem(y + dy, 4) * 2 + lax.rem(core + dc, 2)

    peers = [peer(*d) for d in ((2, 0), (2, 1), (1, 0), (3, 0), (1, 1), (3, 1), (0, 1))]
    from_peers = [peer(*d) for d in ((0, 1), (1, 0), (3, 0), (1, 1), (3, 1), (2, 0), (2, 1))]
    z_order = (4, 3, 5, 2, 6, 1, 7)

    barrier = pltpu.get_barrier_semaphore()

    def hello(r, c):
        pl.semaphore_signal(barrier, inc=1, device_id=(r, c), device_id_type=MESH)

    for j in z_order:
        hello(row, along_z(j) * 4 + x)
    for p in peers:
        hello(p, col)
    hello(*far)
    hello(*right)
    hello(*left)

    def rows_of(block):
        return pl.ds(pl.multiple_of(block * COLS, COLS), COLS)

    probe_load = pltpu.make_async_copy(probe_hbm, probe, load_sem.at[0])
    density_load = pltpu.make_async_copy(density_hbm, density, load_sem.at[1])
    fock_loads = {}
    probe_load.start()
    for i, ahead in enumerate((2, 1, 3, 0)):
        rows = rows_of(along_x(ahead))
        fock_loads[ahead] = pltpu.make_async_copy(fock_hbm.at[:, rows, :], fock.at[:, rows, :], load_sem.at[2 + i])
        fock_loads[ahead].start()

    probe_load.wait()
    for j in range(2):
        probe_t = probe[j].T.reshape(GROUPS, KINDS, 8, COLS)
        for i in range(CUTS):
            start[:, i * KINDS : (i + 1) * KINDS, j * 8 : (j + 1) * 8, :] = probe_t[..., i * WIDE : (i + 1) * WIDE]

    def send(source, target, send_sem, recv_sem, device):
        copy = pltpu.make_async_remote_copy(
            src_ref=source, dst_ref=target, send_sem=send_sem, recv_sem=recv_sem,
            device_id=device, device_id_type=MESH,
        )
        copy.start()

    def landed(target, sem):
        pltpu.make_async_copy(target, target, sem).wait()

    def store(box, value):
        for i in range(CUTS):
            box[i * KINDS : (i + 1) * KINDS] = value[:, i * WIDE : (i + 1) * WIDE].reshape(KINDS, DEPTH, WIDE)

    def stage_x(phase, g):
        if phase == 0:
            vector = start[g]
        else:
            landed(gathered.at[1, g, pl.ds(0, 7)], g_recv.at[0, g])
            vector = gathered[1, g]
        high, low = factors(phase, vector)
        box = chunks.at[phase, g]
        s, r = x_send.at[phase // 2], x_recv.at[phase // 2, g]

        def one(slot, ahead):
            rows = rows_of(along_x(ahead))
            if phase == 0 and g == 0:
                fock_loads[ahead].wait()
                for j in range(2):
                    h, l = split(fock[j, rows, :])
                    fock_high[rows, j * COLS : (j + 1) * COLS] = h
                    fock_low[rows, j * COLS : (j + 1) * COLS] = l
                value = times(high, low, fock_high[rows, :], fock_low[rows, :], 1)
            else:
                block = along_x(ahead)
                value = times(high, low, turned_high[block], turned_low[block], 0)
            store(box.at[slot], value)

        one(0, 2)
        if phase == 0 and g == 0:
            pl.semaphore_wait(barrier, 17)
        send(box.at[0], from_far.at[phase, g], s, r, far)
        one(1, 1)
        send(box.at[1], from_left.at[phase, g], s, r, right)
        one(2, 3)
        send(box.at[2], from_right.at[phase, g], s, r, left)
        one(3, 0)
        if phase == 0:
            if g == 0:
                density_load.start()

            @pl.when(z == row)
            def _():
                box[3] = box[3] + start[g]

    def sum_x(phase, g):
        landed(chunks.at[phase, g, pl.ds(0, 3)], x_recv.at[phase // 2, g])
        near = from_left[phase, g] + from_right[phase, g]
        summed[phase, g] = (chunks[phase, g, 3] + from_far[phase, g]) + near

    def sum_of(a):
        return ((a[0] + a[1]) + (a[2] + a[3])) + ((a[4] + a[5]) + (a[6] + a[7]))

    def stage_spread(g):
        sum_x(0, g)
        for o in z_order:
            j = along_z(o)
            send(summed.at[0, g, j], arrived.at[0, g, z], z_send.at[0], z_recv.at[0, g], (row, j * 4 + x))
        arrived[0, g, z] = summed[0, g, z]

    def stage_collect(g):
        landed(arrived.at[0, g, pl.ds(0, 7)], z_recv.at[0, g])
        mine = blocks.at[g, x, z]
        mine[...] = sum_of(arrived.at[0, g])
        for o in z_order[::-1]:
            j = along_z(o)
            send(mine, mine, zg_send, zg_recv.at[g, min(o, 8 - o) - 1], (row, j * 4 + x))
        forward(g, 0)

    def forward(g, *offsets):
        if offsets[0]:
            landed(arrived.at[0, g, pl.ds(0, len(offsets))], zg_recv.at[g, offsets[0] - 1])
        for o in offsets:
            j = along_z(o)
            piece = blocks.at[g, x, j]
            send(piece, piece, xg_send, xg_recv.at[g, 1], far)
            send(piece, piece, xg_send, xg_recv.at[g, 0], right)
            send(piece, piece, xg_send, xg_recv.at[g, 0], left)

    def adjoint(g, ahead):
        block = along_x(ahead)
        high, low = factors(1, blocks[g, block])
        return times(high, low, density_high[block], density_low[block], 0)

    def stage_own(g):
        sums[g] = adjoint(g, 0)

    def stage_next(g):
        landed(blocks.at[g, pl.ds(0, 2)], xg_recv.at[g, 0])
        sums[g] = sums[g] + (adjoint(g, 1) + adjoint(g, 3))

    def stage_far(g):
        landed(blocks.at[g, 0], xg_recv.at[g, 1])
        store(summed.at[1, g], sums[g] + adjoint(g, 2))
        for p in peers:
            send(summed.at[1, g, p], turned.at[1, g, row], y_send.at[0], y_one.at[g], (p, col))
        turned[1, g, row] = summed[1, g, row]

    def stage_join(g):
        landed(turned.at[1, g, pl.ds(0, 7)], y_one.at[g])
        gather(1, g, sum_of(turned.at[1, g]))

    def gather(phase, g, value):
        mine = gathered.at[phase, g, row]
        mine[...] = value
        for p in peers:
            send(mine, mine, g_send.at[phase - 1], g_recv.at[phase - 1, g], (p, col))

    def to_z(g, block, source):
        @pl.when(block != z)
        def _():
            pltpu.make_async_remote_copy(
                src_ref=source, dst_ref=arrived.at[2, g, z],
                send_sem=z_send.at[1], recv_sem=z_recv.at[1, g],
                device_id=(row, block * 4 + x), device_id_type=MESH,
            ).start()

    def stage_y(g):
        sum_x(2, g)
        for p in peers:
            send(summed.at[2, g, p], turned.at[2, g, row], y_send.at[1], y_recv.at[g, row], (p, col))
        turned[2, g, row] = summed[2, g, row]
        to_z(g, row, summed.at[2, g, row])

    def stage_z(g):
        for p in from_peers:
            piece = turned.at[2, g, p]
            landed(piece, y_recv.at[g, p])
            to_z(g, p, piece)
        arrived[2, g, z] = turned[2, g, z]

    def stage_gather(g):
        landed(arrived.at[2, g, pl.ds(0, 7)], z_recv.at[1, g])
        gather(2, g, sum_of(arrived.at[2, g]) + gathered[1, g, row])

    def stage_turn(g):
        for i in range(ROWS // COLS):
            for j in range(2):
                h, l = split(fock[j, i * COLS : (i + 1) * COLS, :].T)
                turned_high[i, j * COLS : (j + 1) * COLS] = h
                turned_low[i, j * COLS : (j + 1) * COLS] = l

    def stage_density(g):
        if g == 0:
            density_load.wait()

            def part(i, carry):
                for j in range(2):
                    h, l = split(density[j, rows_of(i), :])
                    density_high[i, j * COLS : (j + 1) * COLS] = h
                    density_low[i, j * COLS : (j + 1) * COLS] = l
                return carry

            lax.fori_loop(0, ROWS // COLS, part, 0)

    def stage_out(g):
        landed(gathered.at[2, g, pl.ds(0, 7)], g_recv.at[1, g])
        part, each = gathered[2, g], KINDS * 8
        for j in range(2):
            half = part[:, j * 8 : (j + 1) * 8]
            cuts = [half[i * KINDS : (i + 1) * KINDS].reshape(each, WIDE) for i in range(CUTS)]
            whole = jnp.concatenate(cuts, axis=1) if CUTS > 1 else cuts[0]
            out[j, :, g * each : (g + 1) * each] = whole.T

    def sent():
        every, seven = pl.ds(0, GROUPS), pl.ds(0, 7)
        for i in range(2):
            landed(chunks.at[0, every, pl.ds(0, 3)], x_send.at[i])
            for sem in (y_send, z_send, g_send):
                landed(arrived.at[0, every, seven], sem.at[i])
        landed(arrived.at[0, every, seven], zg_send)
        landed(blocks.at[every, pl.ds(0, 3)], xg_send)

    plan = (
        functools.partial(stage_x, 0),
        stage_turn,
        stage_density,
        stage_spread,
        stage_collect,
        lambda g: forward(g, 1, 7),
        lambda g: forward(g, 2, 6),
        lambda g: forward(g, 3, 5),
        lambda g: forward(g, 4),
        stage_own,
        stage_next,
        stage_far,
        stage_join,
        functools.partial(stage_x, 2),
        stage_y,
        stage_z,
        stage_gather,
        stage_out,
    )
    for turn in ORDER:
        plan[turn // 4](turn % 4)
    sent()


def step(fock, density, probe):
    f32, bf16 = jnp.float32, jnp.bfloat16
    vmem, dma = pltpu.VMEM, pltpu.SemaphoreType.DMA
    each = (PHASES, GROUPS)
    piece = (DEPTH, WIDE)
    return pl.pallas_call(
        kernel,
        out_shape=jax.ShapeDtypeStruct(probe.shape, f32),
        in_specs=[pl.BlockSpec(memory_space=pltpu.HBM)] * 3,
        out_specs=pl.BlockSpec(memory_space=pltpu.VMEM),
        scratch_shapes=[
            vmem(fock.shape, f32), vmem(density.shape, f32), vmem(probe.shape, f32),
            vmem((ROWS, 2 * COLS), bf16), vmem((ROWS, 2 * COLS), bf16),
            vmem((ROWS // COLS, 2 * COLS, COLS), bf16), vmem((ROWS // COLS, 2 * COLS, COLS), bf16),
            vmem((ROWS // COLS, 2 * COLS, COLS), bf16), vmem((ROWS // COLS, 2 * COLS, COLS), bf16),
            vmem((GROUPS, PIECES, *piece), f32),
            vmem((*each, 4, PIECES, *piece), f32),
            vmem((*each, PIECES, *piece), f32),
            vmem((*each, PIECES, *piece), f32), vmem((*each, PIECES, *piece), f32),
            vmem((*each, PIECES, *piece), f32), vmem((*each, PIECES, *piece), f32),
            vmem((*each, 8, *piece), f32), vmem((GROUPS, 4, PIECES, *piece), f32),
            vmem((GROUPS, TALL, COLS), f32), vmem((*each, PIECES, *piece), f32),
            dma((6,)), dma((2,)), dma((2, GROUPS)), dma((2,)), dma((GROUPS,)), dma((GROUPS, PIECES)),
            dma((2,)), dma((2, GROUPS)), dma((2,)), dma((2, GROUPS)),
            dma, dma((GROUPS, 4)), dma, dma((GROUPS, 2)),
        ],
        compiler_params=pltpu.CompilerParams(
            collective_id=0, has_side_effects=True, vmem_limit_bytes=VMEM_LIMIT
        ),
    )(fock, density, probe)


def solution(mesh):
    return jax.shard_map(
        step,
        mesh=mesh,
        in_specs=(P(None, "row", "col"), P(None, "row", "col"), P(None, "col", None)),
        out_specs=P(None, "col", None),
        check_vma=False,
    )
```

```python
import functools

import jax
import jax.numpy as jnp
from jax import lax
from jax.experimental import pallas as pl
from jax.experimental.pallas import tpu as pltpu
from jax.sharding import PartitionSpec as P

MESH = pl.DeviceIdType.MESH
DT = 0.5
ROWS = 1024
COLS = 256
PIECES = 8
DEPTH = 16
GROUPS = 4
CUTS = GROUPS // 2
WIDE = COLS // CUTS
KINDS = PIECES // CUTS
TALL = KINDS * DEPTH
PHASES = 3
VMEM_LIMIT = 54784 * 1024
ORDER = (
    0, 4, 1, 8, 12, 2, 3, 13, 16, 14, 17, 15, 20, 24, 28, 32,
    21, 36, 18, 25, 29, 33, 19, 40, 22, 44, 26, 37, 30, 34, 23, 41,
    45, 27, 48, 38, 31, 35, 39, 42, 46, 49, 52, 43, 47, 50, 53, 51,
    54, 55, 56, 57, 58, 60, 61, 59, 62, 63, 64, 66, 68, 65, 67, 70,
    69, 71,
)


def split(value):
    high = value.astype(jnp.bfloat16)
    return high, (value - high.astype(jnp.float32)).astype(jnp.bfloat16)


def flat(vector):
    parts = [vector[i * KINDS : (i + 1) * KINDS].reshape(TALL, WIDE) for i in range(CUTS)]
    return jnp.concatenate(parts, axis=1) if CUTS > 1 else parts[0]


def factors(phase, vector):
    real, imag = vector[:, :8], vector[:, 8:]
    if phase == 1:
        first, second = (real, imag), (imag, -real)
    else:
        dt = DT if phase == 0 else -DT
        first, second = (-dt * imag, dt * real), (-dt * real, -dt * imag)
    first = flat(jnp.concatenate(first, axis=1))
    second = flat(jnp.concatenate(second, axis=1))
    return split(jnp.concatenate([first, second], axis=1))


def times(high, low, matrix_high, matrix_low, depth_dim):
    dot = functools.partial(
        lax.dot_general,
        dimension_numbers=(((1,), (depth_dim,)), ((), ())),
        preferred_element_type=jnp.float32,
    )
    both = dot(jnp.concatenate([high, low], axis=0), matrix_high)
    return both[:TALL] + (both[TALL:] + dot(high, matrix_low))


def kernel(
    fock_hbm, density_hbm, probe_hbm, out,
    fock, density, probe, fock_high, fock_low, turned_high, turned_low, density_high, density_low,
    start, chunks, from_far, from_left, from_right, summed, turned, arrived, blocks, sums, gathered,
    load_sem, x_send, x_recv, y_send, y_one, y_recv, z_send, z_recv, g_send, g_recv, zg_send, zg_recv, xg_send, xg_recv,
):
    row, col = lax.axis_index("row"), lax.axis_index("col")
    z, x = col // 4, lax.rem(col, 4)
    y, core = row // 2, lax.rem(row, 2)
    right = (row, z * 4 + lax.rem(x + 1, 4))
    left = (row, z * 4 + lax.rem(x + 3, 4))
    far = (row, z * 4 + lax.rem(x + 2, 4))

    def along_x(ahead):
        return lax.rem(x + ahead, 4)

    def along_z(ahead):
        return lax.rem(z + ahead, 8)

    def peer(dy, dc):
        return lax.rem(y + dy, 4) * 2 + lax.rem(core + dc, 2)

    peers = [peer(*d) for d in ((2, 0), (2, 1), (1, 0), (3, 0), (1, 1), (3, 1), (0, 1))]
    waves = [[peer(*d) for d in wave] for wave in (((0, 1),), ((1, 0), (3, 0), (1, 1), (3, 1)), ((2, 0), (2, 1)))]
    wave_of = (2, 2, 1, 1, 1, 1, 0)
    z_order = (4, 3, 5, 2, 6, 1, 7)

    barrier = pltpu.get_barrier_semaphore()

    def hello(r, c):
        pl.semaphore_signal(barrier, inc=1, device_id=(r, c), device_id_type=MESH)

    for j in z_order:
        hello(row, along_z(j) * 4 + x)
    for p in peers:
        hello(p, col)
    hello(*far)
    hello(*right)
    hello(*left)

    def rows_of(block):
        return pl.ds(pl.multiple_of(block * COLS, COLS), COLS)

    probe_load = pltpu.make_async_copy(probe_hbm, probe, load_sem.at[0])
    density_load = pltpu.make_async_copy(density_hbm, density, load_sem.at[1])
    fock_loads = {}
    probe_load.start()
    for i, ahead in enumerate((2, 1, 3, 0)):
        rows = rows_of(along_x(ahead))
        fock_loads[ahead] = pltpu.make_async_copy(fock_hbm.at[:, rows, :], fock.at[:, rows, :], load_sem.at[2 + i])
        fock_loads[ahead].start()

    probe_load.wait()
    for j in range(2):
        probe_t = probe[j].T.reshape(GROUPS, KINDS, 8, COLS)
        for i in range(CUTS):
            start[:, i * KINDS : (i + 1) * KINDS, j * 8 : (j + 1) * 8, :] = probe_t[..., i * WIDE : (i + 1) * WIDE]

    def send(source, target, send_sem, recv_sem, device):
        copy = pltpu.make_async_remote_copy(
            src_ref=source, dst_ref=target, send_sem=send_sem, recv_sem=recv_sem,
            device_id=device, device_id_type=MESH,
        )
        copy.start()

    def landed(target, sem):
        pltpu.make_async_copy(target, target, sem).wait()

    def store(box, value):
        for i in range(CUTS):
            box[i * KINDS : (i + 1) * KINDS] = value[:, i * WIDE : (i + 1) * WIDE].reshape(KINDS, DEPTH, WIDE)

    def stage_x(phase, g):
        if phase == 0:
            vector = start[g]
        else:
            landed(gathered.at[1, g, pl.ds(0, 7)], g_recv.at[0, g])
            vector = gathered[1, g]
        high, low = factors(phase, vector)
        box = chunks.at[phase, g]
        s, r = x_send.at[phase // 2], x_recv.at[phase // 2, g]

        def one(slot, ahead):
            rows = rows_of(along_x(ahead))
            if phase == 0 and g == 0:
                fock_loads[ahead].wait()
                for j in range(2):
                    h, l = split(fock[j, rows, :])
                    fock_high[rows, j * COLS : (j + 1) * COLS] = h
                    fock_low[rows, j * COLS : (j + 1) * COLS] = l
                value = times(high, low, fock_high[rows, :], fock_low[rows, :], 1)
            else:
                block = along_x(ahead)
                value = times(high, low, turned_high[block], turned_low[block], 0)
            store(box.at[slot], value)

        one(0, 2)
        if phase == 0 and g == 0:
            pl.semaphore_wait(barrier, 17)
        send(box.at[0], from_far.at[phase, g], s, r, far)
        one(1, 1)
        send(box.at[1], from_left.at[phase, g], s, r, right)
        one(2, 3)
        send(box.at[2], from_right.at[phase, g], s, r, left)
        one(3, 0)
        if phase == 0:
            if g == 0:
                density_load.start()

            @pl.when(z == row)
            def _():
                box[3] = box[3] + start[g]

    def sum_x(phase, g):
        landed(chunks.at[phase, g, pl.ds(0, 3)], x_recv.at[phase // 2, g])
        near = from_left[phase, g] + from_right[phase, g]
        summed[phase, g] = (chunks[phase, g, 3] + from_far[phase, g]) + near

    def sum_of(a):
        return ((a[0] + a[1]) + (a[2] + a[3])) + ((a[4] + a[5]) + (a[6] + a[7]))

    def stage_spread(g):
        sum_x(0, g)
        for o in z_order:
            j = along_z(o)
            send(summed.at[0, g, j], arrived.at[0, g, z], z_send.at[0], z_recv.at[0, g], (row, j * 4 + x))
        arrived[0, g, z] = summed[0, g, z]

    def stage_collect(g):
        landed(arrived.at[0, g, pl.ds(0, 7)], z_recv.at[0, g])
        mine = blocks.at[g, x, z]
        mine[...] = sum_of(arrived.at[0, g])
        for o in z_order[::-1]:
            j = along_z(o)
            send(mine, mine, zg_send, zg_recv.at[g, min(o, 8 - o) - 1], (row, j * 4 + x))
        forward(g, 0)

    def forward(g, *offsets):
        if offsets[0]:
            landed(arrived.at[0, g, pl.ds(0, len(offsets))], zg_recv.at[g, offsets[0] - 1])
        for o in offsets:
            j = along_z(o)
            piece = blocks.at[g, x, j]
            send(piece, piece, xg_send, xg_recv.at[g, 1], far)
            send(piece, piece, xg_send, xg_recv.at[g, 0], right)
            send(piece, piece, xg_send, xg_recv.at[g, 0], left)

    def adjoint(g, ahead):
        block = along_x(ahead)
        high, low = factors(1, blocks[g, block])
        return times(high, low, density_high[block], density_low[block], 0)

    def stage_own(g):
        sums[g] = adjoint(g, 0)

    def stage_next(g):
        landed(blocks.at[g, pl.ds(0, 2)], xg_recv.at[g, 0])
        sums[g] = sums[g] + (adjoint(g, 1) + adjoint(g, 3))

    def stage_far(g):
        landed(blocks.at[g, 0], xg_recv.at[g, 1])
        store(summed.at[1, g], sums[g] + adjoint(g, 2))
        for p in peers:
            send(summed.at[1, g, p], turned.at[1, g, row], y_send.at[0], y_one.at[g], (p, col))
        turned[1, g, row] = summed[1, g, row]

    def stage_join(g):
        landed(turned.at[1, g, pl.ds(0, 7)], y_one.at[g])
        gather(1, g, sum_of(turned.at[1, g]))

    def gather(phase, g, value):
        mine = gathered.at[phase, g, row]
        mine[...] = value
        for p in peers:
            send(mine, mine, g_send.at[phase - 1], g_recv.at[phase - 1, g], (p, col))

    def to_z(g, block, source):
        @pl.when(block != z)
        def _():
            pltpu.make_async_remote_copy(
                src_ref=source, dst_ref=arrived.at[2, g, z],
                send_sem=z_send.at[1], recv_sem=z_recv.at[1, g],
                device_id=(row, block * 4 + x), device_id_type=MESH,
            ).start()

    def stage_y(g):
        sum_x(2, g)
        for p, wave in zip(peers, wave_of):
            send(summed.at[2, g, p], turned.at[2, g, row], y_send.at[1], y_recv.at[g, wave], (p, col))
        turned[2, g, row] = summed[2, g, row]
        to_z(g, row, summed.at[2, g, row])

    def stage_z(g):
        for i, wave in enumerate(waves):
            landed(arrived.at[2, g, pl.ds(0, len(wave))], y_recv.at[g, i])
            for p in wave:
                to_z(g, p, turned.at[2, g, p])
        arrived[2, g, z] = turned[2, g, z]

    def stage_gather(g):
        landed(arrived.at[2, g, pl.ds(0, 7)], z_recv.at[1, g])
        gather(2, g, sum_of(arrived.at[2, g]) + gathered[1, g, row])

    def stage_turn(g):
        for i in range(ROWS // COLS):
            for j in range(2):
                h, l = split(fock[j, i * COLS : (i + 1) * COLS, :].T)
                turned_high[i, j * COLS : (j + 1) * COLS] = h
                turned_low[i, j * COLS : (j + 1) * COLS] = l

    def stage_density(g):
        if g == 0:
            density_load.wait()

            def part(i, carry):
                for j in range(2):
                    h, l = split(density[j, rows_of(i), :])
                    density_high[i, j * COLS : (j + 1) * COLS] = h
                    density_low[i, j * COLS : (j + 1) * COLS] = l
                return carry

            lax.fori_loop(0, ROWS // COLS, part, 0)

    def stage_out(g):
        landed(gathered.at[2, g, pl.ds(0, 7)], g_recv.at[1, g])
        part, each = gathered[2, g], KINDS * 8
        for j in range(2):
            half = part[:, j * 8 : (j + 1) * 8]
            cuts = [half[i * KINDS : (i + 1) * KINDS].reshape(each, WIDE) for i in range(CUTS)]
            whole = jnp.concatenate(cuts, axis=1) if CUTS > 1 else cuts[0]
            out[j, :, g * each : (g + 1) * each] = whole.T

    def sent():
        every, seven = pl.ds(0, GROUPS), pl.ds(0, 7)
        for i in range(2):
            landed(chunks.at[0, every, pl.ds(0, 3)], x_send.at[i])
            for sem in (y_send, z_send, g_send):
                landed(arrived.at[0, every, seven], sem.at[i])
        landed(arrived.at[0, every, seven], zg_send)
        landed(blocks.at[every, pl.ds(0, 3)], xg_send)

    plan = (
        functools.partial(stage_x, 0),
        stage_turn,
        stage_density,
        stage_spread,
        stage_collect,
        lambda g: forward(g, 1, 7),
        lambda g: forward(g, 2, 6),
        lambda g: forward(g, 3, 5),
        lambda g: forward(g, 4),
        stage_own,
        stage_next,
        stage_far,
        stage_join,
        functools.partial(stage_x, 2),
        stage_y,
        stage_z,
        stage_gather,
        stage_out,
    )
    for turn in ORDER:
        plan[turn // 4](turn % 4)
    sent()


def step(fock, density, probe):
    f32, bf16 = jnp.float32, jnp.bfloat16
    vmem, dma = pltpu.VMEM, pltpu.SemaphoreType.DMA
    each = (PHASES, GROUPS)
    piece = (DEPTH, WIDE)
    return pl.pallas_call(
        kernel,
        out_shape=jax.ShapeDtypeStruct(probe.shape, f32),
        in_specs=[pl.BlockSpec(memory_space=pltpu.HBM)] * 3,
        out_specs=pl.BlockSpec(memory_space=pltpu.VMEM),
        scratch_shapes=[
            vmem(fock.shape, f32), vmem(density.shape, f32), vmem(probe.shape, f32),
            vmem((ROWS, 2 * COLS), bf16), vmem((ROWS, 2 * COLS), bf16),
            vmem((ROWS // COLS, 2 * COLS, COLS), bf16), vmem((ROWS // COLS, 2 * COLS, COLS), bf16),
            vmem((ROWS // COLS, 2 * COLS, COLS), bf16), vmem((ROWS // COLS, 2 * COLS, COLS), bf16),
            vmem((GROUPS, PIECES, *piece), f32),
            vmem((*each, 4, PIECES, *piece), f32),
            vmem((*each, PIECES, *piece), f32),
            vmem((*each, PIECES, *piece), f32), vmem((*each, PIECES, *piece), f32),
            vmem((*each, PIECES, *piece), f32), vmem((*each, PIECES, *piece), f32),
            vmem((*each, 8, *piece), f32), vmem((GROUPS, 4, PIECES, *piece), f32),
            vmem((GROUPS, TALL, COLS), f32), vmem((*each, PIECES, *piece), f32),
            dma((6,)), dma((2,)), dma((2, GROUPS)), dma((2,)), dma((GROUPS,)), dma((GROUPS, 3)),
            dma((2,)), dma((2, GROUPS)), dma((2,)), dma((2, GROUPS)),
            dma, dma((GROUPS, 4)), dma, dma((GROUPS, 2)),
        ],
        compiler_params=pltpu.CompilerParams(
            collective_id=0, has_side_effects=True, vmem_limit_bytes=VMEM_LIMIT
        ),
    )(fock, density, probe)


def solution(mesh):
    return jax.shard_map(
        step,
        mesh=mesh,
        in_specs=(P(None, "row", "col"), P(None, "row", "col"), P(None, "col", None)),
        out_specs=P(None, "col", None),
        check_vma=False,
    )
```
